128 devices in a mesh: batch: 32 (over z, y_hi, x), head: 4 (over y_lo, core).
Axes of the slice: x: 4, y: 4 (y_hi: 2, y_lo: 2; y = y_hi * 2 + y_lo), z: 4, core: 2. Of those that a mesh axis runs over, the one named last changes fastest.
Arguments:
- features: bfloat16 [4096, 24, 512], P(('batch', 'head')), may hold values from -6 to 6
- state_h: bfloat16 [4096, 1024], P(('batch', 'head')), may hold values from -0.8984375 to 0.8984375
- state_c: bfloat16 [4096, 1024], P(('batch', 'head')), may hold values from -4 to 4
- valid: int32 [4096], P(('batch', 'head')), may hold values 0 or 1
- ends: int32 [4096, 24], P(('batch', 'head')), may hold values 0 or 1
- policy: int32 [4096, 1], P(('batch', 'head')), may hold values from 0 to 31; in each aligned block of 32 rows (0 to 31, 32 to 63, ...) at most 2 rows name the same one
- actions: int32 [4096, 16], P(('batch', 'head')), may hold values from 0 to 17
- w_input: bfloat16 [512, 4, 1024], P('batch', None, 'head'), may hold values from -0.25 to 0.25
- w_recur: bfloat16 [1024, 4, 1024], P('batch', None, 'head'), may hold values from -0.1875 to 0.1875
- lstm_bias: float32 [4, 1024], replicated, may hold values from -3 to 5
- w_hidden: bfloat16 [32, 1024, 1024], P('head'), may hold values from -0.1875 to 0.1875
- w_value: bfloat16 [32, 512], P('head'), may hold values from -0.25 to 0.25
- w_advantage: bfloat16 [32, 512, 18], P('head'), may hold values from -0.25 to 0.25
Outputs:
- q_values: float32 [4096, 16, 18], P(('batch', 'head'))
- q_taken: float32 [4096, 16], P(('batch', 'head'))
The draws below stay inside these ranges and needn't reach their ends.
Inputs may be any that keep to these rules, and one draw needn't show every extreme that they name: In the rows of one device no policy appears more than 2 times, and some policy appears exactly 2 times.
All inputs are finite; a program needn't handle non-finite values. No bound on the sum of `valid` or of `ends` on one device may be relied on, other than what follows from the above.
Results may differ from the reference program's by a relative error of at most 0.007.
Values may be sent and summed in bfloat16 or wider, within the bound.
A program may use at most 128 MiB of HBM per device.

```python
import math
import jax
import jax.numpy as jnp
import numpy as np
from jax import lax

E = 512
H = 1024
HID = 512
ACTIONS = 18
POLICIES = 32
SEQ_DEV = 32
BURN = 8
LEARN = 16
CAPP = 2
STEPS = 24
SEQS = 4096


def draw_lstm_bias(key, part):
    base = jax.random.fold_in(key, 41)
    first_key, second_key = jax.random.split(base)
    others = jnp.clip(0.5 * jax.random.normal(first_key, (4, H), jnp.float32), -3.0, 3.0)
    forget = jax.random.uniform(second_key, (H,), jnp.float32, 1.5, 4.5)
    which_row = jnp.arange(4, dtype=jnp.int32)[:, None] == 1
    return jnp.where(which_row, forget[None, :], others).astype(jnp.float32)


def place_ends(values, stream_key, smallest, high):
    place = [jax.random.randint(jax.random.fold_in(stream_key, axis), (), 0, length) for axis, length in enumerate(values.shape)]
    longest = values.shape.index(max(values.shape))
    beside = place[:longest] + [(place[longest] + 1) % values.shape[longest]] + place[longest + 1:]
    return values.at[tuple(place)].set(smallest).at[tuple(beside)].set(high)


def block_scale(stream_key, dims, cuts, smallest, high):
    gain, own = 1.0, jax.random.fold_in(stream_key, 6)
    for axis_at, blocks in cuts:
        heights = jnp.exp(jax.random.uniform(jax.random.fold_in(own, axis_at), (blocks,), jnp.float32, smallest / len(cuts), high / len(cuts)))
        gain = gain * jnp.repeat(heights, dims[axis_at] // blocks).reshape([-1 if axis == axis_at else 1 for axis in range(len(dims))])
    return gain


def routed_block(rng, own, number, rows, number_of, top, bound, skew):
    ranking = jax.random.permutation(rng, number_of)
    crowded, ordinary = shares(number_of, rows * top, bound, skew, True), shares(number_of, rows * top, bound, skew, False)
    places = jnp.arange(number_of)

    def named(lengths, turn):
        used = int((lengths > 0).sum())
        fixed = max(1, used // 4)
        passed = fixed + (places - fixed + turn * (used - fixed)) % max(1, number_of - fixed)
        return jnp.zeros((number_of,), jnp.int32).at[ranking[jnp.where(places < fixed, places, passed)]].set(jnp.asarray(lengths, jnp.int32))

    lengths = jnp.where(number % 4 == 0, named(crowded, number // 4), named(ordinary, number - number // 4 - 1))
    mixed = jax.random.permutation(jax.random.fold_in(own, 3), number_of)
    donor, receiver = mixed[0:number_of // 2 * 2:2], mixed[1:number_of // 2 * 2:2]
    room = jnp.minimum(lengths[donor] - 1, bound - lengths[receiver]) // 2
    room = jnp.where((donor == ranking[0]) | (receiver == ranking[0]) | (lengths[receiver] == 0), 0, jnp.maximum(room, 0))
    passed = jax.random.randint(jax.random.fold_in(own, 4), (number_of // 2,), 0, 1 << 20) % (room + 1)
    lengths = lengths.at[donor].add(-passed).at[receiver].add(passed)
    labels = jnp.searchsorted(jnp.cumsum(lengths), jnp.arange(rows * top), side="right").astype(jnp.int32)
    table = labels.reshape(top, rows).T
    table = table[jax.random.permutation(jax.random.fold_in(own, 1), rows)]
    turn = jax.random.randint(jax.random.fold_in(own, 2), (rows, 1), 0, top)
    return jnp.take_along_axis(table, (jnp.arange(top)[None, :] + turn) % top, axis=1)


def shares(amount, total, bound, skew, full):
    weights = [(1 << 20) // math.isqrt(grade ** skew) + 1 for grade in range(1, amount + 1)]
    largest = bound if full else min(bound, max(-(-total // amount), total * weights[0] // sum(weights)))
    least = 1 if total - largest >= amount - 1 else 0
    given, surplus = [largest] + [least] * (amount - 1), total - largest - least * (amount - 1)
    while surplus > 0:
        movable = [i for i in range(1, amount) if given[i] < largest] or [i for i in range(1, amount) if given[i] < bound]
        mass, budget = sum([weights[i] for i in movable]), surplus
        for i in movable:
            extra = min(bound - given[i], max(1, budget * weights[i] // mass), surplus)
            given[i] = given[i] + extra
            surplus = surplus - extra
    return np.array(given)


def centred(own_key, dims, width, most, pieces=(), kind=jnp.bfloat16):
    gain = block_scale(own_key, dims, pieces, -0.22, 0.18) if pieces else 1.0
    result = jax.random.normal(own_key, dims, jnp.float32) * width * gain
    return jnp.minimum(jnp.maximum(result, -most), most).astype(kind)


def setup_inputs(seed: int = 0) -> dict:
    key_list = jax.random.split(jax.random.key(seed), 14)
    features = centred(key_list[0], (SEQS, STEPS, E), 1.0, 6.0, ((0, 128),))
    state_h = jnp.clip(jax.random.uniform(key_list[1], (SEQS, H), jnp.float32, -0.8984375, 0.8984375) * block_scale(key_list[1], (SEQS, H), ((0, 128),), -0.4, 0.0), -0.8984375, 0.8984375).astype(jnp.bfloat16)
    state_c = centred(key_list[2], (SEQS, H), 1.0, 4.0, ((0, 128),))
    valid = place_ends((jax.random.randint(key_list[3], (SEQS,), 0, 4) < 3).astype(jnp.int32), jax.random.fold_in(key_list[3], 1), 0, 1)
    ends = place_ends((jax.random.randint(key_list[4], (SEQS, STEPS), 0, 12) < 1).astype(jnp.int32), jax.random.fold_in(key_list[4], 1), 0, 1)
    policy_keys = jax.random.split(jax.random.fold_in(key_list[5], 1), SEQS // SEQ_DEV)
    policy_turns = jax.random.permutation(jax.random.fold_in(key_list[5], 3), SEQS // SEQ_DEV)
    policy = jax.vmap(lambda own, number: routed_block(jax.random.fold_in(key_list[5], 2), own, number, SEQ_DEV, POLICIES, 1, CAPP, 2))(policy_keys, policy_turns).reshape((SEQS, 1))
    actions = place_ends(jax.random.randint(key_list[6], (SEQS, LEARN), 0, ACTIONS), jax.random.fold_in(key_list[6], 1), 0, ACTIONS - 1).astype(jnp.int32)
    w_input = centred(key_list[7], (E, 4, H), E ** -0.5, 0.25, ((0, 32), (2, 4)))
    w_recur = centred(key_list[8], (H, 4, H), H ** -0.5, 0.1875, ((0, 32), (2, 4)))
    lstm_bias = draw_lstm_bias(jax.random.fold_in(key_list[13], 71), 0)
    w_hidden = centred(key_list[10], (POLICIES, H, 2 * HID), H ** -0.5, 0.1875, ((0, 4),))
    w_value = centred(key_list[11], (POLICIES, HID), HID ** -0.5, 0.25, ((0, 4),))
    w_advantage = centred(key_list[12], (POLICIES, HID, ACTIONS), HID ** -0.5, 0.25, ((0, 4),))
    return {"features": features, "state_h": state_h, "state_c": state_c, "valid": valid, "ends": ends, "policy": policy, "actions": actions, "w_input": w_input, "w_recur": w_recur, "lstm_bias": lstm_bias, "w_hidden": w_hidden, "w_value": w_value, "w_advantage": w_advantage}


def reference(features, state_h, state_c, valid, ends, policy, actions, w_input, w_recur, lstm_bias, w_hidden, w_value, w_advantage):
    keep_start = valid.astype(jnp.float32)[:, None]
    hidden_state = (state_h.astype(jnp.float32) * keep_start).astype(jnp.bfloat16)
    cell_state = state_c.astype(jnp.float32) * keep_start
    time_major = features.transpose(1, 0, 2)
    keeps = 1.0 - ends.astype(jnp.float32).T
    w_in_flat = w_input.reshape(E, 4 * H)
    w_rec_flat = w_recur.reshape(H, 4 * H)

    def advance(carry, inputs):
        hidden_state, cell_state = carry
        feat_t, keep_t = inputs
        hidden_state = (hidden_state.astype(jnp.float32) * keep_t[:, None]).astype(jnp.bfloat16)
        cell_state = cell_state * keep_t[:, None]
        gates = jnp.dot(feat_t, w_in_flat, preferred_element_type=jnp.float32)
        gates = gates + jnp.dot(hidden_state, w_rec_flat, preferred_element_type=jnp.float32)
        gates = gates.reshape(-1, 4, H) + lstm_bias
        cell_state = jax.nn.sigmoid(gates[:, 1]) * cell_state + jax.nn.sigmoid(gates[:, 0]) * jnp.tanh(gates[:, 2])
        hidden_state = (jax.nn.sigmoid(gates[:, 3]) * jnp.tanh(cell_state)).astype(jnp.bfloat16)
        return (hidden_state, cell_state), hidden_state

    _, outputs = lax.scan(advance, (hidden_state, cell_state), (time_major, keeps))
    learned = outputs[BURN:].transpose(1, 0, 2)

    def one_head(item):
        rows, which = item
        mid = jnp.maximum(jnp.dot(rows, w_hidden[which], preferred_element_type=jnp.float32), 0.0).astype(jnp.bfloat16)
        value = jnp.dot(mid[:, :HID], w_value[which], preferred_element_type=jnp.float32)
        advantage = jnp.dot(mid[:, HID:], w_advantage[which], preferred_element_type=jnp.float32)
        return value[:, None] + advantage - jnp.mean(advantage, axis=-1, keepdims=True)

    q_values = lax.map(one_head, (learned, policy[:, 0].astype(jnp.int32)))
    chosen = actions[:, :, None] == jnp.arange(ACTIONS, dtype=jnp.int32)[None, None, :]
    q_taken = jnp.sum(jnp.where(chosen, q_values, 0.0), axis=-1)
    return q_values, q_taken
```

```python
import jax
import jax.numpy as jnp
from jax import lax
from jax.experimental import pallas as pl
from jax.experimental.pallas import tpu as pltpu
from jax.sharding import PartitionSpec as P

ACTIONS = 18
POLICIES = 32
CAPP = 2
MESH = pl.DeviceIdType.MESH
ORDERS = ("xyz", "yzx", "zxy")
SENDS = 128
F32 = jnp.float32
BF16 = jnp.bfloat16


def here():
    b = lax.axis_index("batch")
    h = lax.axis_index("head")
    return {"x": b % 4, "y": b // 4 % 2 * 2 + h // 2, "z": b // 8, "c": h % 2}


def device(at):
    return (at["z"] * 8 + at["y"] // 2 * 4 + at["x"], at["y"] % 2 * 2 + at["c"])


def shifted(at, axis, by):
    return {**at, axis: (at[axis] + by + 4) % 4}


def entry_barrier(me):
    barrier = pltpu.get_barrier_semaphore()
    other = {**me, "c": 1 - me["c"]}
    peers = [shifted(me, a, d) for a in "xyz" for d in (1, -1, 2)]
    peers += [other, {**other, "y": me["y"] + 1 - 2 * (me["y"] % 2)}]
    for p in peers:
        pl.semaphore_signal(barrier, inc=1, device_id=device(p), device_id_type=MESH)
    pl.semaphore_wait(barrier, len(peers))


class Copies:
    def __init__(self, send_sem, recv_sem):
        self.sems = (send_sem, recv_sem)
        self.sent = []

    def send(self, src, dst, to):
        k = len(self.sent)
        copy = pltpu.make_async_remote_copy(
            src_ref=src,
            dst_ref=dst,
            send_sem=self.sems[0].at[k],
            recv_sem=self.sems[1].at[k],
            device_id=device(to),
            device_id_type=MESH,
        )
        copy.start()
        self.sent.append(copy)
        return copy

    def push(self, ref, to):
        return self.send(ref, ref, to)


def gather(me, shard, full, copies):
    other = {**me, "c": 1 - me["c"]}
    crossed = []

    def region(part, at, free=None, half=None):
        z, x = at["z"], at["x"]
        y = (at["y"] // 2, at["y"] % 2)
        if free == "y":
            y = (slice(None) if half is None else half, slice(None))
        elif free is not None:
            span = slice(None) if half is None else pl.ds(2 * half, 2)
            z, x = (span, x) if free == "z" else (z, span)
        return full.at[me["c"], z, y[0], y[1], x, :, pl.ds(16 * part, 16), :]

    def cross(ref):
        crossed.append(copies.push(ref, other))

    full[me["c"], me["z"], me["y"] // 2, me["y"] % 2, me["x"]] = shard[...]
    first, line, third, relay = {}, {}, {}, {}
    for d in (1, -1, 2):
        for k, (a, b, c) in enumerate(ORDERS):
            own = shard.at[:, pl.ds(16 * k, 16), :]
            first[k, d] = copies.send(own, region(k, me), shifted(me, a, d))

    def along_last(k, m, at):
        a, b, c = ORDERS[k]
        for d in (1, -1):
            third[k, m, d] = copies.push(region(k, at, free=a), shifted(me, c, d))

    for k, (a, b, c) in enumerate(ORDERS):
        for d in (1, -1, 2):
            first[k, d].wait_recv()
        for d in (1, -1):
            line[k, d] = copies.push(region(k, me, free=a), shifted(me, b, d))
        along_last(k, 0, me)
        cross(region(k, me, free=a))
    for k, (a, b, c) in enumerate(ORDERS):
        for m, d in ((1, 1), (2, -1)):
            line[k, d].wait_recv()
            at = shifted(me, b, -d)
            relay[k, d] = copies.push(region(k, at, free=a, half=(1 - d) // 2), shifted(me, b, d))
            along_last(k, m, at)
            cross(region(k, at, free=a))
    for k, (a, b, c) in enumerate(ORDERS):
        for d in (1, -1):
            relay[k, d].wait_recv()
        at = shifted(me, b, 2)
        along_last(k, 3, at)
        cross(region(k, at, free=a))
    relay = {}
    offsets = (0, -1, 1, 2)
    for m in range(4):
        for k, (a, b, c) in enumerate(ORDERS):
            for d in (1, -1):
                third[k, m, d].wait_recv()
                at = shifted(shifted(me, b, offsets[m]), c, -d)
                relay[k, m, d] = copies.push(region(k, at, free=a, half=(1 - d) // 2), shifted(me, c, d))
                cross(region(k, at, free=a))
    for m in range(4):
        for k, (a, b, c) in enumerate(ORDERS):
            for d in (1, -1):
                relay[k, m, d].wait_recv()
            cross(region(k, shifted(shifted(me, b, offsets[m]), c, 2), free=a))
    for copy in crossed:
        copy.wait_recv()


def sigmoid(v):
    return 0.5 * jnp.tanh(0.5 * v) + 0.5


def core_kernel(
    shard, feat, state_h, state_c, valid, ends, bias, out, full, pre, even, odd, cell, keep, send_sem, recv_sem
):
    me = here()
    steps, seqs = 24, 32
    entry_barrier(me)
    copies = Copies(send_sem, recv_sem)
    alive = 1.0 - ends[...].astype(F32)
    for t in range(steps):
        keep[t] = jnp.broadcast_to(alive[:, t : t + 1], (seqs, 128))
    keep[steps] = jnp.ones((seqs, 128), F32)
    start = jnp.broadcast_to(valid[...].astype(F32), (seqs, 128)) * keep[0]
    start = jnp.concatenate([start] * 8, axis=1)
    even[...] = (state_h[...].astype(F32) * start).astype(BF16)
    cell[...] = state_c[...].astype(F32) * start
    gather(me, shard, full, copies)

    @pl.loop(0, 4)
    def _(hp):
        for pair in range(2):
            tiles = [
                full[hp % 2, :, :, hp // 2, :, 2 * pair + g, 0:16, :].reshape(512, 256) for g in range(2)
            ]
            got = jnp.dot(feat[...], jnp.concatenate(tiles, axis=1), preferred_element_type=F32)
            for g in range(2):
                at = 2 * pair + g
                pre[hp * 4 + at] = got[:, g * 256 : g * 256 + 256] + bias[hp, at : at + 1, :]

    def step(t, src, dst, save):
        h = src[...]
        alive = keep[t + 1]
        alive = jnp.concatenate([alive, alive], axis=1)
        rows = pl.ds(pl.multiple_of(t * seqs, seqs), seqs)
        for hp in range(4):
            gate = []
            for g in range(4):
                w = full[hp % 2, :, :, hp // 2, :, g, 16:48, :].reshape(1024, 256)
                gate.append(jnp.dot(h, w, preferred_element_type=F32) + pre[hp * 4 + g, rows, :])
            cols = slice(hp * 256, hp * 256 + 256)
            c = sigmoid(gate[1]) * cell[:, cols] + sigmoid(gate[0]) * jnp.tanh(gate[2])
            new = sigmoid(gate[3]) * jnp.tanh(c)
            cell[:, cols] = c * alive
            dst[:, cols] = (new * alive).astype(BF16)
            if save:
                out[t - 8, :, cols] = new.astype(BF16)

    def two(save):
        def body(i, _):
            step(2 * i, even, odd, save)
            step(2 * i + 1, odd, even, save)
            return 0

        return body

    lax.fori_loop(0, 4, two(False), 0)
    lax.fori_loop(4, 12, two(True), 0)
    for copy in copies.sent:
        copy.wait_send()


def recurrent_core(w_input, w_recur, features, state_h, state_c, valid, ends, lstm_bias):
    shard = jnp.concatenate([w_input, w_recur], axis=0).transpose(1, 0, 2)
    feat = features.transpose(1, 0, 2).reshape(-1, features.shape[2])
    bias = lstm_bias.reshape(4, 4, 256).transpose(1, 0, 2)
    vmem = pl.BlockSpec(memory_space=pltpu.VMEM)
    return pl.pallas_call(
        core_kernel,
        out_shape=jax.ShapeDtypeStruct((16, 32, 1024), BF16),
        in_specs=[vmem] * 7,
        out_specs=vmem,
        scratch_shapes=[
            pltpu.VMEM((2, 4, 2, 2, 4, 4, 48, 256), BF16),
            pltpu.VMEM((16, 768, 256), F32),
            pltpu.VMEM((32, 1024), BF16),
            pltpu.VMEM((32, 1024), BF16),
            pltpu.VMEM((32, 1024), F32),
            pltpu.VMEM((25, 32, 128), F32),
            pltpu.SemaphoreType.DMA((SENDS,)),
            pltpu.SemaphoreType.DMA((SENDS,)),
        ],
        compiler_params=pltpu.CompilerParams(
            collective_id=0, has_side_effects=True, vmem_limit_bytes=48 * 2**20
        ),
        name="core",
    )(shard, feat, state_h, state_c, valid[:, None], ends, bias)


def slot_table(owners, per_source, capacity, policies):
    count = owners.shape[0]
    sources = count // per_source
    place = jnp.arange(count, dtype=jnp.int32)
    anchor = place // per_source
    before = (
        (owners[:, None] == owners[None, :])
        & (anchor[:, None] == anchor[None, :])
        & (place[None, :] < place[:, None])
    )
    rank = jnp.sum(before.astype(jnp.int32), axis=1)
    target = owners * (sources * capacity) + anchor * capacity + rank
    total = policies * sources * capacity
    return (jnp.arange(total, dtype=jnp.int32)[:, None] == target[None, :]).astype(jnp.bfloat16)


def shards(
    features,
    state_h,
    state_c,
    valid,
    ends,
    policy,
    actions,
    w_input,
    w_recur,
    lstm_bias,
    w_hidden,
    w_value,
    w_advantage,
):
    seq_dev, steps, width_e = features.shape
    width_h = state_h.shape[1]
    learn = actions.shape[1]
    learned = recurrent_core(w_input, w_recur, features, state_h, state_c, valid, ends, lstm_bias)
    table = slot_table(policy[:, 0], seq_dev, CAPP, POLICIES)
    packed = jnp.einsum("ks,tsu->ktu", table, learned, preferred_element_type=jnp.float32).astype(
        jnp.bfloat16
    )
    packed = packed.reshape(POLICIES, CAPP, learn, width_h)
    routed = lax.all_to_all(packed, "head", split_axis=0, concat_axis=1, tiled=True)
    local_heads, slots = (routed.shape[0], routed.shape[1])
    rows = routed.reshape(local_heads, slots * learn, width_h)
    mid = jnp.einsum("prh,phk->prk", rows, w_hidden, preferred_element_type=jnp.float32)
    mid = jnp.maximum(mid, 0.0).astype(jnp.bfloat16)
    branch = w_value.shape[1]
    value = jnp.einsum(
        "prk,pk->pr", mid[:, :, :branch], w_value, preferred_element_type=jnp.float32
    )
    advantage = jnp.einsum(
        "prk,pka->pra", mid[:, :, branch:], w_advantage, preferred_element_type=jnp.float32
    )
    q_local = value[:, :, None] + advantage - jnp.mean(advantage, axis=-1, keepdims=True)
    q_local = q_local.reshape(local_heads, slots, learn, ACTIONS)
    returned = lax.all_to_all(
        q_local.astype(jnp.bfloat16), "head", split_axis=1, concat_axis=0, tiled=True
    ).astype(q_local.dtype)
    own_table = slot_table(policy[:, 0], seq_dev, CAPP, POLICIES).astype(jnp.float32)
    q_values = jnp.dot(
        own_table.T,
        returned.reshape(POLICIES * CAPP, learn * ACTIONS),
        precision=lax.Precision.HIGHEST,
    ).reshape(seq_dev, learn, ACTIONS)
    chosen = actions[:, :, None] == jnp.arange(ACTIONS, dtype=jnp.int32)[None, None, :]
    q_taken = jnp.sum(jnp.where(chosen, q_values, 0.0), axis=-1)
    return (q_values, q_taken)


def solution(mesh):
    return jax.shard_map(
        shards,
        mesh=mesh,
        in_specs=(
            P(("batch", "head"), None, None),
            P(("batch", "head"), None),
            P(("batch", "head"), None),
            P(("batch", "head")),
            P(("batch", "head"), None),
            P(("batch", "head"), None),
            P(("batch", "head"), None),
            P("batch", None, "head"),
            P("batch", None, "head"),
            P(),
            P("head", None, None),
            P("head", None),
            P("head", None, None),
        ),
        out_specs=(P(("batch", "head"), None, None), P(("batch", "head"), None)),
        check_vma=False,
    )
```

```python
import jax
import jax.numpy as jnp
from jax import lax
from jax.experimental import pallas as pl
from jax.experimental.pallas import tpu as pltpu
from jax.sharding import PartitionSpec as P

ACTIONS = 18
MESH = pl.DeviceIdType.MESH
ORDERS = ("xyz", "yzx", "zxy")
SENDS = 128
F32 = jnp.float32
BF16 = jnp.bfloat16


def here():
    b = lax.axis_index("batch")
    h = lax.axis_index("head")
    return {"x": b % 4, "y": b // 4 % 2 * 2 + h // 2, "z": b // 8, "c": h % 2}


def device(at):
    return (at["z"] * 8 + at["y"] // 2 * 4 + at["x"], at["y"] % 2 * 2 + at["c"])


def shifted(at, axis, by):
    return {**at, axis: (at[axis] + by + 4) % 4}


def entry_barrier(me):
    barrier = pltpu.get_barrier_semaphore()
    other = {**me, "c": 1 - me["c"]}
    peers = [shifted(me, a, d) for a in "xyz" for d in (1, -1, 2)]
    peers += [other, {**other, "y": me["y"] + 1 - 2 * (me["y"] % 2)}]
    for p in peers:
        pl.semaphore_signal(barrier, inc=1, device_id=device(p), device_id_type=MESH)
    pl.semaphore_wait(barrier, len(peers))


class Copies:
    def __init__(self, send_sem, recv_sem):
        self.sems = (send_sem, recv_sem)
        self.sent = []

    def send(self, src, dst, to):
        k = len(self.sent)
        copy = pltpu.make_async_remote_copy(
            src_ref=src,
            dst_ref=dst,
            send_sem=self.sems[0].at[k],
            recv_sem=self.sems[1].at[k],
            device_id=device(to),
            device_id_type=MESH,
        )
        copy.start()
        self.sent.append(copy)
        return copy

    def push(self, ref, to):
        return self.send(ref, ref, to)


def gather(me, shard, full, copies, meanwhile):
    other = {**me, "c": 1 - me["c"]}
    crossed = []

    def region(part, at, free=None, half=None):
        z, x = at["z"], at["x"]
        y = (at["y"] // 2, at["y"] % 2)
        if free == "y":
            y = (slice(None) if half is None else half, slice(None))
        elif free is not None:
            span = slice(None) if half is None else pl.ds(2 * half, 2)
            z, x = (span, x) if free == "z" else (z, span)
        return full.at[me["c"], z, y[0], y[1], x, :, pl.ds(16 * part, 16), :]

    def cross(ref):
        crossed.append(copies.push(ref, other))

    full[me["c"], me["z"], me["y"] // 2, me["y"] % 2, me["x"]] = shard[...]
    first, line, third, relay = {}, {}, {}, {}
    for d in (1, -1, 2):
        for k, (a, b, c) in enumerate(ORDERS):
            own = shard.at[:, pl.ds(16 * k, 16), :]
            first[k, d] = copies.send(own, region(k, me), shifted(me, a, d))
    meanwhile()

    def along_last(k, m, at):
        a, b, c = ORDERS[k]
        for d in (1, -1):
            third[k, m, d] = copies.push(region(k, at, free=a), shifted(me, c, d))

    for k, (a, b, c) in enumerate(ORDERS):
        for d in (1, -1, 2):
            first[k, d].wait_recv()
        for d in (1, -1):
            line[k, d] = copies.push(region(k, me, free=a), shifted(me, b, d))
        along_last(k, 0, me)
        cross(region(k, me, free=a))
    for k, (a, b, c) in enumerate(ORDERS):
        for m, d in ((1, 1), (2, -1)):
            line[k, d].wait_recv()
            at = shifted(me, b, -d)
            relay[k, d] = copies.push(region(k, at, free=a, half=(1 - d) // 2), shifted(me, b, d))
            along_last(k, m, at)
            cross(region(k, at, free=a))
    for k, (a, b, c) in enumerate(ORDERS):
        for d in (1, -1):
            relay[k, d].wait_recv()
        at = shifted(me, b, 2)
        along_last(k, 3, at)
        cross(region(k, at, free=a))
    relay = {}
    offsets = (0, -1, 1, 2)
    for m in range(4):
        for k, (a, b, c) in enumerate(ORDERS):
            for d in (1, -1):
                third[k, m, d].wait_recv()
                at = shifted(shifted(me, b, offsets[m]), c, -d)
                relay[k, m, d] = copies.push(region(k, at, free=a, half=(1 - d) // 2), shifted(me, c, d))
                cross(region(k, at, free=a))
    for m in range(4):
        for k, (a, b, c) in enumerate(ORDERS):
            for d in (1, -1):
                relay[k, m, d].wait_recv()
            cross(region(k, shifted(shifted(me, b, offsets[m]), c, 2), free=a))
    for copy in crossed:
        copy.wait_recv()


def sigmoid(v):
    return 0.5 * jnp.tanh(0.5 * v) + 0.5


def iota(shape, dim):
    return lax.broadcasted_iota(jnp.int32, shape, dim)


def ones_where(mask, dtype):
    return jnp.where(mask, 1.0, 0.0).astype(dtype)


def prepare(table, wv, wa, head, keep, info, value_w, adv_w, spread, lane_group, chosen):
    ends = table[:, 0:24].astype(F32)
    for t in range(24):
        keep[t] = jnp.broadcast_to(1.0 - ends[:, t : t + 1], (32, 128))
    keep[24] = jnp.ones((32, 128), F32)
    policy = jnp.broadcast_to(table[:, 40:41], (32, 256)).astype(F32)
    seq = iota((32, 256), 1) & 31
    row = iota((32, 256), 0)
    across = jnp.sum(jnp.where(row == seq, policy, 0.0), axis=0, keepdims=True)
    same = policy == across
    rank_across = jnp.sum(ones_where(same & (row < seq), F32), axis=0, keepdims=True)
    info[head] = jnp.concatenate(
        [jnp.broadcast_to(across, (8, 256)), jnp.broadcast_to(rank_across, (8, 256))], axis=0
    )

    def finish():
        lane = iota((32, 128), 1)
        earlier = same[:, 0:128] & (lane < row[:, 0:128])
        rank = jnp.sum(ones_where(earlier, F32), axis=1, keepdims=True)
        number = table[:, 40:41]
        base = (number >> 2).astype(F32) * 32.0 + rank * 8.0
        group = (number & 3).astype(F32)
        each = ones_where((iota((512, 32), 0) >> 4) == iota((512, 32), 1), BF16)
        place = iota((512, 128), 0) & 15

        def per_row(column):
            wide = jnp.broadcast_to(column, (32, 128)).astype(BF16)
            return jnp.dot(each, wide, preferred_element_type=F32)

        slot = per_row(base) + ((place >> 3) * 16 + (place & 7)).astype(F32)
        slot = jnp.concatenate([slot, slot], axis=1)
        spread[...] = ones_where(slot == iota((512, 256), 1).astype(F32), BF16)
        lanes = iota((512, 128), 1)
        lane_group[...] = ones_where((lanes >> 5).astype(F32) == per_row(group), F32)
        taken = jnp.dot(each, table[:, 24:40].astype(F32).astype(BF16), preferred_element_type=F32)
        at = iota((512, 16), 1) == (iota((512, 16), 0) & 15)
        taken = jnp.sum(jnp.where(at, taken, 0.0), axis=1, keepdims=True)
        chosen[...] = ones_where(jnp.broadcast_to(taken, (512, 128)) == lanes.astype(F32), F32)
        adv_w[...] = jnp.zeros(adv_w.shape, BF16)
        adv_w[:, :, 0:ACTIONS] = wa[...]
        for p in range(8):
            line = wv[p : p + 1, :].astype(F32)
            value_w[p] = jnp.broadcast_to(line, (128, 512)).T.astype(BF16)

    return finish


def core_kernel(
    shard,
    table,
    bias,
    wv,
    wa,
    feat_hbm,
    state_h,
    state_c,
    wh_hbm,
    q_out,
    taken_out,
    full,
    pre,
    even,
    odd,
    cell,
    keep,
    feat,
    hidden_w,
    learned,
    packed,
    info,
    pick,
    value_w,
    adv_w,
    spread,
    lane_group,
    chosen,
    answers,
    replies,
    local_sem,
    send_sem,
    recv_sem,
    route_send,
    route_recv,
):
    me = here()
    seqs = 32
    head = me["y"] % 2 * 2 + me["c"]
    other = {**me, "c": 1 - me["c"]}
    facing = {**me, "y": me["y"] + 1 - 2 * (me["y"] % 2)}
    across = {**facing, "c": 1 - me["c"]}
    head_of = lambda at: at["y"] % 2 * 2 + at["c"]
    loads = [pltpu.make_async_copy(feat_hbm, feat, local_sem.at[8])]
    loads[0].start()
    entry_barrier(me)
    copies = Copies(send_sem, recv_sem)
    told = []

    def meanwhile():
        for p in range(8):
            loads.append(pltpu.make_async_copy(wh_hbm.at[p], hidden_w.at[p], local_sem.at[p]))
            loads[-1].start()
        rest = prepare(table, wv, wa, head, keep, info, value_w, adv_w, spread, lane_group, chosen)
        start = jnp.broadcast_to(table[:, 41:42].astype(F32), (seqs, 128)) * keep[0]
        start = jnp.concatenate([start] * 8, axis=1)
        even[...] = (state_h[...].astype(F32) * start).astype(BF16)
        cell[...] = state_c[...].astype(F32) * start
        rest()
        for to in (other, facing, across):
            told.append(copies.push(info.at[head], to))

    gather(me, shard, full, copies, meanwhile)
    loads[0].wait()
    for copy in told:
        copy.wait_recv()
    lane = iota((128, 256), 1)
    row = iota((128, 256), 0)
    step_at = (lane >> 5) == (row & 7)
    for s in range(4):
        mine = info[s, 0:1, :] == ((row >> 4) + 8 * head).astype(F32)
        cap = info[s, 8:9, :] == ((row >> 3) & 1).astype(F32)
        pick[s] = ones_where(mine & cap & step_at, BF16)

    for hp in range(4):
        for pair in range(2):
            tiles = [
                full[hp % 2, :, :, hp // 2, :, 2 * pair + g, 0:16, :].reshape(512, 256) for g in range(2)
            ]
            got = jnp.dot(feat[...], jnp.concatenate(tiles, axis=1), preferred_element_type=F32)
            for g in range(2):
                at = 2 * pair + g
                line = bias[at : at + 1, hp * 256 : hp * 256 + 256]
                pre[hp * 4 + at] = got[:, g * 256 : g * 256 + 256] + line

    def step(t, src, dst, save):
        h = src[...]
        alive = keep[t + 1]
        alive = jnp.concatenate([alive, alive], axis=1)
        rows = pl.ds(pl.multiple_of(t * seqs, seqs), seqs)
        for hp in range(4):
            gate = []
            for g in range(4):
                w = full[hp % 2, :, :, hp // 2, :, g, 16:48, :].reshape(1024, 256)
                gate.append(jnp.dot(h, w, preferred_element_type=F32) + pre[hp * 4 + g, rows, :])
            cols = slice(hp * 256, hp * 256 + 256)
            c = sigmoid(gate[1]) * cell[:, cols] + sigmoid(gate[0]) * jnp.tanh(gate[2])
            new = sigmoid(gate[3]) * jnp.tanh(c)
            cell[:, cols] = c * alive
            dst[:, cols] = (new * alive).astype(BF16)
            if save:
                learned[head, t - 8, :, cols] = new.astype(BF16)

    def route(kind, i, owner, to):
        ref = learned.at[head_of(owner), i]
        return pltpu.make_async_remote_copy(
            src_ref=ref,
            dst_ref=ref,
            send_sem=route_send.at[kind, i],
            recv_sem=route_recv.at[kind, i],
            device_id=device(to),
            device_id_type=MESH,
        )

    def send_out(i):
        route(1, i, me, facing).start()
        route(0, i, me, other).start()

    def hand_on(i):
        route(1, i, me, facing).wait_recv()
        route(2, i, facing, other).start()

    def burn(i, _):
        step(2 * i, even, odd, False)
        step(2 * i + 1, odd, even, False)
        return 0

    lag = 4

    def learn(i, _):
        @pl.when(i > 0)
        def _():
            send_out(2 * i - 1)

        @pl.when(2 * i >= lag)
        def _():
            hand_on(2 * i - lag)
            hand_on(2 * i - lag + 1)

        step(2 * i + 8, even, odd, True)
        send_out(2 * i)
        step(2 * i + 9, odd, even, True)
        return 0

    lax.fori_loop(0, 4, burn, 0)
    lax.fori_loop(0, 8, learn, 0)
    send_out(15)

    def pack(s, half):
        rows = learned[s, 8 * half : 8 * half + 8].reshape(256, 1024)
        got = jnp.dot(pick[s], rows, preferred_element_type=F32).astype(BF16)
        packed[:, (2 * s + half) * 16 : (2 * s + half) * 16 + 16, :] = got.reshape(8, 16, 1024)

    for i in range(16 - lag, 16):
        hand_on(i)
    for i in range(16):
        route(0, i, me, other).wait_recv()
        route(2, i, facing, other).wait_recv()
    for s in range(4):
        for half in range(2):
            pack(s, half)
    for load in loads[1:]:
        load.wait()
    valid_lane = iota((128, 128), 1) < ACTIONS
    for quad in range(2):
        total = None
        for j in range(4):
            p = 4 * quad + j
            mid = jnp.dot(packed[p], hidden_w[p], preferred_element_type=F32)
            mid = jnp.maximum(mid, 0.0).astype(BF16)
            value = jnp.dot(mid[:, 0:512], value_w[p], preferred_element_type=F32)
            adv = jnp.dot(mid[:, 512:1024], adv_w[p], preferred_element_type=F32)
            q = value + adv - jnp.sum(adv, axis=1, keepdims=True) * (1.0 / ACTIONS)
            q = jnp.where(valid_lane, q, 0.0)
            if j:
                q = pltpu.roll(q, 32 * j, 1)
            total = q if total is None else total + q
        for s in range(4):
            answers[s, 32 * quad : 32 * quad + 32, :] = total[32 * s : 32 * s + 32].astype(BF16)
    replies[head] = answers[head]
    back = []
    for to in (across, facing, other):
        back.append(copies.send(answers.at[head_of(to)], replies.at[head], to))
    for copy in back:
        copy.wait_recv()
    found = jnp.dot(spread[...], replies[...].reshape(256, 128), preferred_element_type=F32)
    found = (found * lane_group[...]).astype(BF16)
    fold = ones_where((iota((128, 128), 0) & 31) == iota((128, 128), 1), BF16)
    q = jnp.dot(found, fold, preferred_element_type=F32)
    q_out[...] = q.reshape(32, 16, 128)[:, :, 0:ACTIONS]
    picked = jnp.sum(q * chosen[...], axis=1, keepdims=True)
    at = iota((512, 16), 1) == (iota((512, 16), 0) & 15)
    picked = jnp.where(at, jnp.broadcast_to(picked, (512, 16)), 0.0).astype(BF16)
    collect = ones_where((iota((32, 512), 1) >> 4) == iota((32, 512), 0), BF16)
    taken_out[...] = jnp.dot(collect, picked, preferred_element_type=F32)
    for i in range(16):
        route(0, i, me, other).wait_send()
        route(1, i, me, facing).wait_send()
        route(2, i, facing, other).wait_send()
    for copy in copies.sent:
        copy.wait_send()


def shards(
    features,
    state_h,
    state_c,
    valid,
    ends,
    policy,
    actions,
    w_input,
    w_recur,
    lstm_bias,
    w_hidden,
    w_value,
    w_advantage,
):
    shard = jnp.concatenate([w_input, w_recur], axis=0).transpose(1, 0, 2)
    feat = features.transpose(1, 0, 2).reshape(-1, features.shape[2])
    table = jnp.concatenate([ends, actions, policy, valid[:, None]], axis=1)
    vmem = pl.BlockSpec(memory_space=pltpu.VMEM)
    hbm = pl.BlockSpec(memory_space=pl.ANY)
    dma = pltpu.SemaphoreType.DMA
    return pl.pallas_call(
        core_kernel,
        out_shape=(
            jax.ShapeDtypeStruct((32, 16, ACTIONS), F32),
            jax.ShapeDtypeStruct((32, 16), F32),
        ),
        in_specs=[vmem] * 5 + [hbm] + [vmem] * 2 + [hbm],
        out_specs=(vmem, vmem),
        scratch_shapes=[
            pltpu.VMEM((2, 4, 2, 2, 4, 4, 48, 256), BF16),
            pltpu.VMEM((16, 768, 256), F32),
            pltpu.VMEM((32, 1024), BF16),
            pltpu.VMEM((32, 1024), BF16),
            pltpu.VMEM((32, 1024), F32),
            pltpu.VMEM((25, 32, 128), F32),
            pltpu.VMEM((768, 512), BF16),
            pltpu.VMEM((8, 1024, 1024), BF16),
            pltpu.VMEM((4, 16, 32, 1024), BF16),
            pltpu.VMEM((8, 128, 1024), BF16),
            pltpu.VMEM((4, 16, 256), F32),
            pltpu.VMEM((4, 128, 256), BF16),
            pltpu.VMEM((8, 512, 128), BF16),
            pltpu.VMEM((8, 512, 128), BF16),
            pltpu.VMEM((512, 256), BF16),
            pltpu.VMEM((512, 128), F32),
            pltpu.VMEM((512, 128), F32),
            pltpu.VMEM((4, 64, 128), BF16),
            pltpu.VMEM((4, 64, 128), BF16),
            dma((9,)),
            dma((SENDS,)),
            dma((SENDS,)),
            dma((3, 16)),
            dma((3, 16)),
        ],
        compiler_params=pltpu.CompilerParams(
            collective_id=0, has_side_effects=True, vmem_limit_bytes=60 * 2**20
        ),
        name="core",
    )(shard, table, lstm_bias, w_value, w_advantage, feat, state_h, state_c, w_hidden)


def solution(mesh):
    return jax.shard_map(
        shards,
        mesh=mesh,
        in_specs=(
            P(("batch", "head"), None, None),
            P(("batch", "head"), None),
            P(("batch", "head"), None),
            P(("batch", "head")),
            P(("batch", "head"), None),
            P(("batch", "head"), None),
            P(("batch", "head"), None),
            P("batch", None, "head"),
            P("batch", None, "head"),
            P(),
            P("head", None, None),
            P("head", None),
            P("head", None, None),
        ),
        out_specs=(P(("batch", "head"), None, None), P(("batch", "head"), None)),
        check_vma=False,
    )
```

```python
import jax
import jax.numpy as jnp
from jax import lax
from jax.experimental import pallas as pl
from jax.experimental.pallas import tpu as pltpu
from jax.sharding import PartitionSpec as P

ACTIONS = 18
MESH = pl.DeviceIdType.MESH
ORDERS = ("xyz", "yzx", "zxy")
SENDS = 176
F32 = jnp.float32
BF16 = jnp.bfloat16


def here():
    b = lax.axis_index("batch")
    h = lax.axis_index("head")
    return {"x": b % 4, "y": b // 4 % 2 * 2 + h // 2, "z": b // 8, "c": h % 2}


def device(at):
    return (at["z"] * 8 + at["y"] // 2 * 4 + at["x"], at["y"] % 2 * 2 + at["c"])


def shifted(at, axis, by):
    return {**at, axis: (at[axis] + by + 4) % 4}


def entry_barrier(me):
    barrier = pltpu.get_barrier_semaphore()
    other = {**me, "c": 1 - me["c"]}
    peers = [shifted(me, a, d) for a in "xyz" for d in (1, -1, 2)]
    peers += [other, {**other, "y": me["y"] + 1 - 2 * (me["y"] % 2)}]
    for p in peers:
        pl.semaphore_signal(barrier, inc=1, device_id=device(p), device_id_type=MESH)
    pl.semaphore_wait(barrier, len(peers))


class Copies:
    def __init__(self, send_sem, recv_sem):
        self.sems = (send_sem, recv_sem)
        self.sent = []

    def send(self, src, dst, to):
        k = len(self.sent)
        copy = pltpu.make_async_remote_copy(
            src_ref=src,
            dst_ref=dst,
            send_sem=self.sems[0].at[k],
            recv_sem=self.sems[1].at[k],
            device_id=device(to),
            device_id_type=MESH,
        )
        copy.start()
        self.sent.append(copy)
        return copy

    def push(self, ref, to):
        return self.send(ref, ref, to)


def gather(me, shard, full, copies, meanwhile):
    other = {**me, "c": 1 - me["c"]}
    crossed = []

    def region(part, at, free=None, half=None):
        z, x = at["z"], at["x"]
        y = (at["y"] // 2, at["y"] % 2)
        if free == "y":
            y = (slice(None) if half is None else half, slice(None))
        elif free is not None:
            span = slice(None) if half is None else pl.ds(2 * half, 2)
            z, x = (span, x) if free == "z" else (z, span)
        return full.at[me["c"], z, y[0], y[1], x, :, pl.ds(16 * part, 16), :]

    def cross(ref):
        crossed.append(copies.push(ref, other))

    def own(k):
        return shard.at[:, pl.ds(16 * k, 16), :]

    first, relay = {}, {}
    line = {(k, d): [] for k in range(3) for d in (1, -1)}
    third = {(k, m, d): [] for k in range(3) for m in range(4) for d in (1, -1)}
    for d in (1, -1, 2):
        for k, (a, b, c) in enumerate(ORDERS):
            first[k, d] = copies.send(own(k), region(k, me), shifted(me, a, d))

    def along_both(k, at, src):
        a, b, c = ORDERS[k]
        for d in (1, -1):
            line[k, d].append(copies.send(src, region(k, at), shifted(me, b, d)))
        for d in (1, -1):
            third[k, 0, d].append(copies.send(src, region(k, at), shifted(me, c, d)))

    def along_last(k, m, at):
        a, b, c = ORDERS[k]
        for d in (1, -1):
            third[k, m, d].append(copies.push(region(k, at, free=a), shifted(me, c, d)))

    for k in range(3):
        along_both(k, me, own(k))
    full[me["c"], me["z"], me["y"] // 2, me["y"] % 2, me["x"]] = shard[...]
    meanwhile()
    for d in (1, -1, 2):
        for k, (a, b, c) in enumerate(ORDERS):
            first[k, d].wait_recv()
            at = shifted(me, a, -d)
            along_both(k, at, region(k, at))
    for k, (a, b, c) in enumerate(ORDERS):
        cross(region(k, me, free=a))
    for k, (a, b, c) in enumerate(ORDERS):
        for m, d in ((1, 1), (2, -1)):
            for copy in line[k, d]:
                copy.wait_recv()
            at = shifted(me, b, -d)
            relay[k, d] = copies.push(region(k, at, free=a, half=(1 - d) // 2), shifted(me, b, d))
            along_last(k, m, at)
            cross(region(k, at, free=a))
    for k, (a, b, c) in enumerate(ORDERS):
        for d in (1, -1):
            relay[k, d].wait_recv()
        at = shifted(me, b, 2)
        along_last(k, 3, at)
        cross(region(k, at, free=a))
    relay = {}
    offsets = (0, -1, 1, 2)
    for m in range(4):
        for k, (a, b, c) in enumerate(ORDERS):
            for d in (1, -1):
                for copy in third[k, m, d]:
                    copy.wait_recv()
                at = shifted(shifted(me, b, offsets[m]), c, -d)
                relay[k, m, d] = copies.push(region(k, at, free=a, half=(1 - d) // 2), shifted(me, c, d))
                cross(region(k, at, free=a))
    for m in range(4):
        for k, (a, b, c) in enumerate(ORDERS):
            for d in (1, -1):
                relay[k, m, d].wait_recv()
            cross(region(k, shifted(shifted(me, b, offsets[m]), c, 2), free=a))
    for copy in crossed:
        copy.wait_recv()


def sigmoid(v):
    return 0.5 * jnp.tanh(0.5 * v) + 0.5


def iota(shape, dim):
    return lax.broadcasted_iota(jnp.int32, shape, dim)


def ones_where(mask, dtype):
    return jnp.where(mask, 1.0, 0.0).astype(dtype)


def prepare(ends, actions, policy, valid, small, wv, wa, wide, head, keep, info, value_w, adv_w, spread, group):
    small[...] = jnp.zeros((128, 128), F32)
    small[0:24, 0:32] = ends[...].astype(F32)
    small[24:40, 0:32] = actions[...].astype(F32)
    small[40:41, 0:32] = policy[...].astype(F32)
    small[41:42, 0:32] = valid[...].astype(F32)
    by_seq = small[...].T
    for t in range(24):
        keep[t] = jnp.broadcast_to(1.0 - by_seq[0:32, t : t + 1], (32, 128))
    keep[24] = jnp.ones((32, 128), F32)
    rows = small[24:48, :]
    rows = rows + pltpu.roll(rows, 32, 1) + pltpu.roll(rows, 64, 1) + pltpu.roll(rows, 96, 1)
    across = rows[16:17, :]
    same = jnp.broadcast_to(by_seq[0:32, 40:41], (32, 128)) == across
    earlier = iota((32, 128), 0) < (iota((32, 128), 1) & 31)
    rank = jnp.sum(ones_where(same & earlier, F32), axis=0, keepdims=True)
    info[head] = jnp.concatenate(
        [jnp.broadcast_to(jnp.concatenate([v, v], axis=1), (8, 256)) for v in (across, rank)], axis=0
    )
    start = jnp.broadcast_to(by_seq[0:32, 41:42], (32, 128)) * keep[0]

    def finish():
        lane = iota((1, 512), 1)
        step = lane >> 5
        number = jnp.concatenate([across] * 4, axis=1).astype(jnp.int32)
        slot = (number >> 2) * 32 + (step >> 3) * 16 + (step & 7)
        slot = slot + jnp.concatenate([rank] * 4, axis=1).astype(jnp.int32) * 8
        spread[...] = ones_where(iota((256, 512), 0) == slot, BF16)
        group[...] = ones_where((iota((128, 512), 0) >> 5) == (number & 3), F32)
        picks = jnp.concatenate([rows[0:16, :]] * 4, axis=1)
        on = iota((16, 512), 0) == (iota((16, 512), 1) >> 5)
        for p in range(8):
            line = wv[p : p + 1, :].astype(F32)
            value_w[p] = jnp.broadcast_to(line, (128, 512)).T.astype(BF16)
        wide[...] = jnp.zeros((1024, 128), F32)
        for a in range(ACTIONS):
            line = wa[a].astype(F32)
            for col in range(4):
                wide[pl.ds(256 * col + a, 8, stride=32), :] = line[:, 128 * col : 128 * col + 128]
        for p in range(8):
            part = [wide[256 * col + 32 * p : 256 * col + 32 * p + 32, :] for col in range(4)]
            part = jnp.concatenate([jnp.concatenate(part, axis=1), jnp.zeros((96, 512), F32)], axis=0)
            adv_w[p] = part.T.astype(BF16)
        return jnp.sum(jnp.where(on, picks, 0.0), axis=0, keepdims=True)

    return start, finish


def core_kernel(
    w_in,
    w_rec,
    ends,
    actions,
    policy,
    valid,
    bias,
    wv,
    wa,
    state_h,
    state_c,
    feat_hbm,
    wh_hbm,
    q_out,
    taken_out,
    shard,
    full,
    pre,
    even,
    odd,
    cell,
    keep,
    raw,
    feat,
    hidden_w,
    learned,
    packed,
    small,
    wide,
    info,
    pick,
    value_w,
    adv_w,
    spread,
    group,
    act,
    answers,
    replies,
    local_sem,
    send_sem,
    recv_sem,
    route_send,
    route_recv,
):
    me = here()
    seqs = 32
    head = me["y"] % 2 * 2 + me["c"]
    other = {**me, "c": 1 - me["c"]}
    facing = {**me, "y": me["y"] + 1 - 2 * (me["y"] % 2)}
    diagonal = {**facing, "c": 1 - me["c"]}
    head_of = lambda at: at["y"] % 2 * 2 + at["c"]
    loads = [pltpu.make_async_copy(feat_hbm, raw, local_sem.at[8])]
    loads[0].start()
    for g in range(4):
        shard[g, 0:16, :] = w_in[:, g, :]
        shard[g, 16:48, :] = w_rec[:, g, :]
    entry_barrier(me)
    copies = Copies(send_sem, recv_sem)
    told = []

    def meanwhile():
        for p in range(8):
            loads.append(pltpu.make_async_copy(wh_hbm.at[p], hidden_w.at[p], local_sem.at[p]))
            loads[-1].start()
        start, rest = prepare(
            ends, actions, policy, valid, small, wv, wa, wide, head, keep, info, value_w, adv_w, spread, group
        )
        start = jnp.concatenate([start] * 8, axis=1)
        even[...] = (state_h[...].astype(F32) * start).astype(BF16)
        cell[...] = state_c[...].astype(F32) * start
        act[...] = jnp.broadcast_to(rest(), (8, 512))
        for to in (other, facing, diagonal):
            told.append(copies.push(info.at[head], to))
        loads[0].wait()
        for part in range(3):
            row = iota((256, 768), 0)
            order = ones_where(iota((256, 768), 1) == (row & 31) * 24 + (row >> 5) + 8 * part, BF16)
            got = jnp.dot(order, raw[...], preferred_element_type=F32)
            feat[256 * part : 256 * part + 256, :] = got.astype(BF16)

    gather(me, shard, full, copies, meanwhile)
    for copy in told:
        copy.wait_recv()
    lane = iota((128, 256), 1)
    row = iota((128, 256), 0)
    step_at = (lane >> 5) == (row & 7)
    for s in range(4):
        mine = info[s, 0:1, :] == ((row >> 4) + 8 * head).astype(F32)
        cap = info[s, 8:9, :] == ((row >> 3) & 1).astype(F32)
        pick[s] = ones_where(mine & cap & step_at, BF16)

    def project(rows):
        f = feat[rows, :]
        for hp in range(4):
            for pair in range(2):
                tiles = [
                    full[hp % 2, :, :, hp // 2, :, 2 * pair + g, 0:16, :].reshape(512, 256)
                    for g in range(2)
                ]
                got = jnp.dot(f, jnp.concatenate(tiles, axis=1), preferred_element_type=F32)
                for g in range(2):
                    at = 2 * pair + g
                    line = bias[at : at + 1, hp * 256 : hp * 256 + 256]
                    pre[hp * 4 + at, rows, :] = got[:, g * 256 : g * 256 + 256] + line

    project(slice(0, 12 * seqs))

    def step(t, src, dst, save):
        h = src[...]
        h = jnp.concatenate([h, h, h, h], axis=0)
        alive = keep[t + 1]
        alive = jnp.concatenate([alive, alive], axis=1)
        rows = pl.ds(pl.multiple_of(t * seqs, seqs), seqs)
        for hp in range(4):
            gate = []
            for g in range(4):
                w = full[hp % 2, :, :, hp // 2, :, g, 16:48, :].reshape(1024, 256)
                got = jnp.dot(h, w, preferred_element_type=F32)[0:seqs]
                gate.append(got + pre[hp * 4 + g, rows, :])
            cols = slice(hp * 256, hp * 256 + 256)
            c = sigmoid(gate[1]) * cell[:, cols] + sigmoid(gate[0]) * jnp.tanh(gate[2])
            new = sigmoid(gate[3]) * jnp.tanh(c)
            cell[:, cols] = c * alive
            dst[:, cols] = (new * alive).astype(BF16)
            if save:
                learned[head, t - 8, :, cols] = new.astype(BF16)

    def route(kind, i, owner, to):
        ref = learned.at[head_of(owner), i]
        return pltpu.make_async_remote_copy(
            src_ref=ref,
            dst_ref=ref,
            send_sem=route_send.at[kind, i],
            recv_sem=route_recv.at[kind, i],
            device_id=device(to),
            device_id_type=MESH,
        )

    def send_out(i):
        route(1, i, me, facing).start()
        route(0, i, me, other).start()

    def hand_on(i):
        route(1, i, me, facing).wait_recv()
        route(2, i, facing, other).start()

    def burn(i, _):
        for u in range(4):
            src, dst = (odd, even) if u % 2 else (even, odd)
            step(4 * i + u, src, dst, False)
        return 0

    lag = 6

    def learn(i, _):
        for u in range(4):
            at = 4 * i + u
            if u == 0:

                @pl.when(i > 0)
                def _():
                    send_out(at - 1)

            else:
                send_out(at - 1)

            @pl.when(at >= lag)
            def _():
                hand_on(at - lag)

            src, dst = (odd, even) if u % 2 else (even, odd)
            step(at + 8, src, dst, True)

        @pl.when(i < 3)
        def _():
            project(pl.ds(pl.multiple_of((4 * i + 12) * seqs, 128), 128))

        return 0

    lax.fori_loop(0, 2, burn, 0)
    lax.fori_loop(0, 4, learn, 0)
    send_out(15)

    def pack(s, half):
        rows = learned[s, 8 * half : 8 * half + 8].reshape(256, 1024)
        got = jnp.dot(pick[s], rows, preferred_element_type=F32).astype(BF16)
        packed[:, (2 * s + half) * 16 : (2 * s + half) * 16 + 16, :] = got.reshape(8, 16, 1024)

    for load in loads[1:]:
        load.wait()
    for i in range(16 - lag, 16):
        hand_on(i)
    for i in range(8):
        route(0, i, me, other).wait_recv()
        route(2, i, facing, other).wait_recv()
    for s in range(4):
        pack(s, 0)
    for i in range(8, 16):
        route(0, i, me, other).wait_recv()
        route(2, i, facing, other).wait_recv()
    for s in range(4):
        pack(s, 1)
    valid_lane = iota((128, 128), 1) < ACTIONS
    for quad in range(2):
        total = None
        for j in range(4):
            p = 4 * quad + j
            mid = jnp.dot(packed[p], hidden_w[p], preferred_element_type=F32)
            mid = jnp.maximum(mid, 0.0).astype(BF16)
            value = jnp.dot(mid[:, 0:512], value_w[p], preferred_element_type=F32)
            adv = jnp.dot(mid[:, 512:1024], adv_w[p], preferred_element_type=F32)
            q = value + adv - jnp.sum(adv, axis=1, keepdims=True) * (1.0 / ACTIONS)
            q = jnp.where(valid_lane, q, 0.0)
            if j:
                q = pltpu.roll(q, 32 * j, 1)
            total = q if total is None else total + q
        for s in range(4):
            answers[s, 32 * quad : 32 * quad + 32, :] = total[32 * s : 32 * s + 32].astype(BF16)
    replies[head] = answers[head]
    back = []
    for to in (diagonal, facing, other):
        back.append(copies.send(answers.at[head_of(to)], replies.at[head], to))
    for copy in back:
        copy.wait_recv()
    got = replies[...].reshape(256, 128).astype(F32).T.astype(BF16)
    found = jnp.dot(got, spread[...], preferred_element_type=F32) * group[...]
    found = found[0:32] + found[32:64] + found[64:96] + found[96:128]
    chosen = jnp.where(iota((32, 512), 0).astype(F32) == act[0:1, :], found, 0.0)
    taken = jnp.sum(chosen, axis=0, keepdims=True)
    for t in range(16):
        tile, off = t // 4 * 128, t % 4 * 32
        now = found[0:24, tile : tile + 128]
        mine = jnp.broadcast_to(taken[:, tile : tile + 128], (8, 128))
        if off:
            now = pltpu.roll(now, 128 - off, 1)
            mine = pltpu.roll(mine, 128 - off, 1)
        q_out[pl.ds(t, ACTIONS, stride=16), :] = now[0:ACTIONS, 0:32]
        taken_out[t : t + 1, :] = mine[0:1, 0:32]
    for i in range(16):
        route(0, i, me, other).wait_send()
        route(1, i, me, facing).wait_send()
        route(2, i, facing, other).wait_send()
    for copy in copies.sent:
        copy.wait_send()


def shards(
    features,
    state_h,
    state_c,
    valid,
    ends,
    policy,
    actions,
    w_input,
    w_recur,
    lstm_bias,
    w_hidden,
    w_value,
    w_advantage,
):
    vmem = pl.BlockSpec(memory_space=pltpu.VMEM)
    hbm = pl.BlockSpec(memory_space=pl.ANY)
    dma = pltpu.SemaphoreType.DMA
    q, taken = pl.pallas_call(
        core_kernel,
        out_shape=(
            jax.ShapeDtypeStruct((ACTIONS * 16, 32), F32),
            jax.ShapeDtypeStruct((16, 32), F32),
        ),
        in_specs=[vmem] * 11 + [hbm] * 2,
        out_specs=(vmem, vmem),
        scratch_shapes=[
            pltpu.VMEM((4, 48, 256), BF16),
            pltpu.VMEM((2, 4, 2, 2, 4, 4, 48, 256), BF16),
            pltpu.VMEM((16, 768, 256), F32),
            pltpu.VMEM((32, 1024), BF16),
            pltpu.VMEM((32, 1024), BF16),
            pltpu.VMEM((32, 1024), F32),
            pltpu.VMEM((25, 32, 128), F32),
            pltpu.VMEM((768, 512), BF16),
            pltpu.VMEM((768, 512), BF16),
            pltpu.VMEM((8, 1024, 1024), BF16),
            pltpu.VMEM((4, 16, 32, 1024), BF16),
            pltpu.VMEM((8, 128, 1024), BF16),
            pltpu.VMEM((128, 128), F32),
            pltpu.VMEM((1024, 128), F32),
            pltpu.VMEM((4, 16, 256), F32),
            pltpu.VMEM((4, 128, 256), BF16),
            pltpu.VMEM((8, 512, 128), BF16),
            pltpu.VMEM((8, 512, 128), BF16),
            pltpu.VMEM((256, 512), BF16),
            pltpu.VMEM((128, 512), F32),
            pltpu.VMEM((8, 512), F32),
            pltpu.VMEM((4, 64, 128), BF16),
            pltpu.VMEM((4, 64, 128), BF16),
            dma((9,)),
            dma((SENDS,)),
            dma((SENDS,)),
            dma((3, 16)),
            dma((3, 16)),
        ],
        compiler_params=pltpu.CompilerParams(
            collective_id=0, has_side_effects=True, vmem_limit_bytes=60 * 2**20
        ),
        name="core",
    )(
        w_input,
        w_recur,
        ends.T,
        actions.T,
        policy.T,
        valid[None, :],
        lstm_bias,
        w_value,
        w_advantage.transpose(2, 0, 1),
        state_h,
        state_c,
        features.reshape(-1, features.shape[2]),
        w_hidden,
    )
    return q.reshape(ACTIONS, 16, 32).transpose(2, 1, 0), taken.T


def solution(mesh):
    return jax.shard_map(
        shards,
        mesh=mesh,
        in_specs=(
            P(("batch", "head"), None, None),
            P(("batch", "head"), None),
            P(("batch", "head"), None),
            P(("batch", "head")),
            P(("batch", "head"), None),
            P(("batch", "head"), None),
            P(("batch", "head"), None),
            P("batch", None, "head"),
            P("batch", None, "head"),
            P(),
            P("head", None, None),
            P("head", None),
            P("head", None, None),
        ),
        out_specs=(P(("batch", "head"), None, None), P(("batch", "head"), None)),
        check_vma=False,
    )
```

```python
import jax
import jax.numpy as jnp
from jax import lax
from jax.experimental import pallas as pl
from jax.experimental.pallas import tpu as pltpu
from jax.sharding import PartitionSpec as P

ACTIONS = 18
MESH = pl.DeviceIdType.MESH
ORDERS = ("xyz", "yzx", "zxy")
SENDS = 176
F32 = jnp.float32
BF16 = jnp.bfloat16


def here():
    b = lax.axis_index("batch")
    h = lax.axis_index("head")
    return {"x": b % 4, "y": b // 4 % 2 * 2 + h // 2, "z": b // 8, "c": h % 2}


def device(at):
    return (at["z"] * 8 + at["y"] // 2 * 4 + at["x"], at["y"] % 2 * 2 + at["c"])


def shifted(at, axis, by):
    return {**at, axis: (at[axis] + by + 4) % 4}


def greet(me):
    barrier = pltpu.get_barrier_semaphore()
    other = {**me, "c": 1 - me["c"]}
    peers = [shifted(me, a, d) for a in "xyz" for d in (1, -1, 2)]
    peers += [other, {**other, "y": me["y"] + 1 - 2 * (me["y"] % 2)}]
    for p in peers:
        pl.semaphore_signal(barrier, inc=1, device_id=device(p), device_id_type=MESH)
    return lambda: pl.semaphore_wait(barrier, len(peers))


class Copies:
    def __init__(self, send_sem, recv_sem):
        self.sems = (send_sem, recv_sem)
        self.sent = []

    def send(self, src, dst, to):
        k = len(self.sent)
        copy = pltpu.make_async_remote_copy(
            src_ref=src,
            dst_ref=dst,
            send_sem=self.sems[0].at[k],
            recv_sem=self.sems[1].at[k],
            device_id=device(to),
            device_id_type=MESH,
        )
        copy.start()
        self.sent.append(copy)
        return copy

    def push(self, ref, to):
        return self.send(ref, ref, to)


def gather(me, shard, full, copies, meanwhile, later):
    other = {**me, "c": 1 - me["c"]}
    crossed = []

    def region(part, at, free=None, half=None):
        z, x = at["z"], at["x"]
        y = (at["y"] // 2, at["y"] % 2)
        if free == "y":
            y = (slice(None) if half is None else half, slice(None))
        elif free is not None:
            span = slice(None) if half is None else pl.ds(2 * half, 2)
            z, x = (span, x) if free == "z" else (z, span)
        return full.at[me["c"], z, y[0], y[1], x, :, pl.ds(16 * part, 16), :]

    def cross(ref):
        crossed.append(copies.push(ref, other))

    def own(k):
        return shard.at[:, pl.ds(16 * k, 16), :]

    first, relay = {}, {}
    line = {(k, d): [] for k in range(3) for d in (1, -1)}
    third = {(k, m, d): [] for k in range(3) for m in range(4) for d in (1, -1)}
    for d in (1, -1, 2):
        for k, (a, b, c) in enumerate(ORDERS):
            first[k, d] = copies.send(own(k), region(k, me), shifted(me, a, d))

    def along_both(k, at, src):
        a, b, c = ORDERS[k]
        for d in (1, -1):
            line[k, d].append(copies.send(src, region(k, at), shifted(me, b, d)))
        for d in (1, -1):
            third[k, 0, d].append(copies.send(src, region(k, at), shifted(me, c, d)))

    def along_last(k, m, at):
        a, b, c = ORDERS[k]
        for d in (1, -1):
            third[k, m, d].append(copies.push(region(k, at, free=a), shifted(me, c, d)))

    for k in range(3):
        along_both(k, me, own(k))
    full[me["c"], me["z"], me["y"] // 2, me["y"] % 2, me["x"]] = shard[...]
    meanwhile()
    for d in (1, -1, 2):
        for k, (a, b, c) in enumerate(ORDERS):
            first[k, d].wait_recv()
            at = shifted(me, a, -d)
            along_both(k, at, region(k, at))
    for k, (a, b, c) in enumerate(ORDERS):
        cross(region(k, me, free=a))
    for k, (a, b, c) in enumerate(ORDERS):
        for m, d in ((1, 1), (2, -1)):
            for copy in line[k, d]:
                copy.wait_recv()
            at = shifted(me, b, -d)
            relay[k, d] = copies.push(region(k, at, free=a, half=(1 - d) // 2), shifted(me, b, d))
            along_last(k, m, at)
            cross(region(k, at, free=a))
    for k, (a, b, c) in enumerate(ORDERS):
        for d in (1, -1):
            relay[k, d].wait_recv()
        at = shifted(me, b, 2)
        along_last(k, 3, at)
        cross(region(k, at, free=a))
    later()
    relay = {}
    offsets = (0, -1, 1, 2)
    for m in range(4):
        for k, (a, b, c) in enumerate(ORDERS):
            for d in (1, -1):
                for copy in third[k, m, d]:
                    copy.wait_recv()
                at = shifted(shifted(me, b, offsets[m]), c, -d)
                relay[k, m, d] = copies.push(region(k, at, free=a, half=(1 - d) // 2), shifted(me, c, d))
                cross(region(k, at, free=a))
    for m in range(4):
        for k, (a, b, c) in enumerate(ORDERS):
            for d in (1, -1):
                relay[k, m, d].wait_recv()
            cross(region(k, shifted(shifted(me, b, offsets[m]), c, 2), free=a))
    for copy in crossed:
        copy.wait_recv()


def sigmoid(v):
    return 0.5 * jnp.tanh(0.5 * v) + 0.5


def iota(shape, dim):
    return lax.broadcasted_iota(jnp.int32, shape, dim)


def ones_where(mask, dtype):
    return jnp.where(mask, 1.0, 0.0).astype(dtype)


def prepare(ends, actions, policy, valid, small, wv, wa, wide, head, keep, info, value_w, adv_w, spread, group):
    small[...] = jnp.zeros((128, 128), F32)
    small[0:24, 0:32] = ends[...].astype(F32)
    small[24:40, 0:32] = actions[...].astype(F32)
    small[40:41, 0:32] = policy[...].astype(F32)
    small[41:42, 0:32] = valid[...].astype(F32)
    by_seq = small[...].T
    for t in range(24):
        keep[t] = jnp.broadcast_to(1.0 - by_seq[0:32, t : t + 1], (32, 128))
    keep[24] = jnp.ones((32, 128), F32)

    def tiled():
        rows = small[24:48, :]
        return rows + pltpu.roll(rows, 32, 1) + pltpu.roll(rows, 64, 1) + pltpu.roll(rows, 96, 1)

    across = tiled()[16:17, :]
    same = jnp.broadcast_to(by_seq[0:32, 40:41], (32, 128)) == across
    earlier = iota((32, 128), 0) < (iota((32, 128), 1) & 31)
    rank = jnp.sum(ones_where(same & earlier, F32), axis=0, keepdims=True)
    info[head] = jnp.concatenate(
        [jnp.broadcast_to(jnp.concatenate([v, v], axis=1), (8, 256)) for v in (across, rank)], axis=0
    )
    start = jnp.broadcast_to(by_seq[0:32, 41:42], (32, 128)) * keep[0]

    def finish():
        rows, across, rank = tiled(), info[head, 0:1, 0:128], info[head, 8:9, 0:128]
        lane = iota((1, 512), 1)
        step = lane >> 5
        number = jnp.concatenate([across] * 4, axis=1).astype(jnp.int32)
        slot = (number >> 2) * 32 + (step >> 3) * 16 + (step & 7)
        slot = slot + jnp.concatenate([rank] * 4, axis=1).astype(jnp.int32) * 8
        spread[...] = ones_where(iota((256, 512), 0) == slot, BF16)
        group[...] = ones_where((iota((128, 512), 0) >> 5) == (number & 3), F32)
        picks = jnp.concatenate([rows[0:16, :]] * 4, axis=1)
        on = iota((16, 512), 0) == (iota((16, 512), 1) >> 5)
        for p in range(8):
            line = wv[p : p + 1, :].astype(F32)
            value_w[p] = jnp.broadcast_to(line, (128, 512)).T.astype(BF16)
        wide[...] = jnp.zeros((1024, 128), F32)
        for a in range(ACTIONS):
            line = wa[a].astype(F32)
            for col in range(4):
                wide[pl.ds(256 * col + a, 8, stride=32), :] = line[:, 128 * col : 128 * col + 128]
        for p in range(8):
            part = [wide[256 * col + 32 * p : 256 * col + 32 * p + 32, :] for col in range(4)]
            part = jnp.concatenate([jnp.concatenate(part, axis=1), jnp.zeros((96, 512), F32)], axis=0)
            adv_w[p] = part.T.astype(BF16)
        return jnp.sum(jnp.where(on, picks, 0.0), axis=0, keepdims=True)

    return start, finish


class Unit:
    def __init__(self, number, accs):
        self.number = number
        self.gates, self.spare, self.wide = accs
        self.turn = 0

    def push(self, tile, slot):
        pltpu.matmul_push_rhs(tile, staging_register=slot, mxu_index=self.number)

    def run(self, acc, pairs):
        for rows, tile in pairs:
            self.push(tile, self.turn)
            pltpu.matmul_acc_lhs(acc, rows, load_staged_rhs=self.turn)
            self.turn = 1 - self.turn
        return acc


def accumulators(number):
    acc = pltpu.ACC(number)
    return (
        [acc((32, 256), F32) for _ in range(8)],
        acc((96, 256), F32),
        [acc((128, 256), F32) for _ in range(5)],
    )


def core_kernel(*refs):
    pl.run_scoped(lambda first, second: core(refs, (Unit(0, first), Unit(1, second))), accumulators(0), accumulators(1))


def core(refs, units):
    given, (q_out, taken_out), held = refs[:13], refs[13:15], refs[15:26]
    w_in, w_rec, ends, actions, policy, valid, bias, wv, wa, state_h, state_c = held
    (
        shard, full, pre, even, odd, cell, keep, feat, hidden_w, learned, packed, small, wide, info, pick,
        value_w, adv_w, spread, group, act, answers, replies, local_sem, send_sem, recv_sem, route_send, route_recv,
    ) = refs[26:]
    wh_hbm = given[12]
    me = here()
    met = greet(me)
    for unit in units:
        for acc in unit.gates + [unit.spare] + unit.wide:
            pltpu.matmul_pop(acc)
    seqs = 32
    head = me["y"] % 2 * 2 + me["c"]
    other = {**me, "c": 1 - me["c"]}
    facing = {**me, "y": me["y"] + 1 - 2 * (me["y"] % 2)}
    diagonal = {**facing, "c": 1 - me["c"]}
    head_of = lambda at: at["y"] % 2 * 2 + at["c"]
    raw = packed.at[0:6, :, 0:512]
    loads = [pltpu.make_async_copy(given[k], ref, local_sem.at[8 + k]) for k, ref in enumerate(held + (raw,))]
    for load in loads:
        load.start()
    for load in loads[0:2]:
        load.wait()
    for g in range(4):
        shard[g, 0:16, :] = w_in[:, g, :]
        shard[g, 16:48, :] = w_rec[:, g, :]
    met()
    copies = Copies(send_sem, recv_sem)
    told = []
    rest = []
    weights = [pltpu.make_async_copy(wh_hbm.at[p], hidden_w.at[p], local_sem.at[p]) for p in range(8)]

    def meanwhile():
        for load in loads[2:]:
            load.wait()
        start, finish = prepare(
            ends, actions, policy, valid, small, wv, wa, wide, head, keep, info, value_w, adv_w, spread, group
        )
        rest.append(finish)
        start = jnp.concatenate([start] * 8, axis=1)
        even[...] = (state_h[...].astype(F32) * start).astype(BF16)
        cell[...] = state_c[...].astype(F32) * start
        for to in (other, facing, diagonal):
            told.append(copies.push(info.at[head], to))
        for load in weights:
            load.start()

    def later():
        act[...] = jnp.broadcast_to(rest[0](), (8, 512))
        for part in range(6):
            row = iota((128, 768), 0)
            order = ones_where(iota((128, 768), 1) == (row & 31) * 24 + (row >> 5) + 4 * part, BF16)
            for n, unit in enumerate(units):
                cols = slice(256 * n, 256 * n + 256)
                pairs = [
                    (order[:, 256 * k : 256 * k + 256], packed[2 * k : 2 * k + 2, :, cols].reshape(256, 256))
                    for k in range(3)
                ]
                got = pltpu.matmul_pop(unit.run(unit.wide[part % 4], pairs))
                feat[128 * part : 128 * part + 128, cols] = got.astype(BF16)

    gather(me, shard, full, copies, meanwhile, later)
    for copy in told:
        copy.wait_recv()
    lane = iota((128, 256), 1)
    row = iota((128, 256), 0)
    step_at = (lane >> 5) == (row & 7)
    for s in range(4):
        mine = info[s, 0:1, :] == ((row >> 4) + 8 * head).astype(F32)
        cap = info[s, 8:9, :] == ((row >> 3) & 1).astype(F32)
        pick[s] = ones_where(mine & cap & step_at, BF16)

    def project(start):
        rows = pl.ds(start, 128)
        f = [feat[rows, 256 * k : 256 * k + 256] for k in range(2)]
        for n in range(16):
            hp, g = n // 4, n % 4
            unit = units[n % 2]
            pairs = [
                (f[k], full[hp % 2, 2 * k : 2 * k + 2, :, hp // 2, :, g, 0:16, :].reshape(256, 256))
                for k in range(2)
            ]
            got = pltpu.matmul_pop(unit.run(unit.wide[n // 2 % 4], pairs))
            pre[n, rows, :] = got + bias[g : g + 1, hp * 256 : hp * 256 + 256]

    for part in range(3):
        project(128 * part)

    tiles = [(hp, pair, 0) for hp in range(4) for pair in range(2)]
    tiles += [(hp, pair, k) for hp in range(4) for k in range(1, 4) for pair in range(2)]

    def stage(i):
        hp, pair, k = tiles[i % 32]
        for q, unit in enumerate(units):
            w = full[hp % 2, k, :, hp // 2, :, 2 * pair + q, 16:48, :].reshape(256, 256)
            unit.push(w, i % 2)

    def multiply(src, first, last, ahead=True):
        for i in range(first, last):
            if ahead or i + 1 < last:
                stage(i + 1)
            hp, pair, k = tiles[i]
            h = src[:, 256 * k : 256 * k + 256]
            for unit in units:
                pltpu.matmul_acc_lhs(unit.gates[2 * hp + pair], h, load_staged_rhs=i % 2)
            h = jnp.concatenate([h, h, h], axis=0)
            for unit in units:
                pltpu.matmul_acc_lhs(unit.spare, h)

    def settle(t, hp, dst, save):
        rows = pl.ds(pl.multiple_of(t * seqs, seqs), seqs)
        alive = keep[t + 1]
        alive = jnp.concatenate([alive, alive], axis=1)
        gate = [pltpu.matmul_pop(units[g % 2].gates[2 * hp + g // 2]) for g in range(4)]
        gate = [gate[g] + pre[hp * 4 + g, rows, :] for g in range(4)]
        cols = slice(hp * 256, hp * 256 + 256)
        c = sigmoid(gate[1]) * cell[:, cols] + sigmoid(gate[0]) * jnp.tanh(gate[2])
        new = sigmoid(gate[3]) * jnp.tanh(c)
        cell[:, cols] = c * alive
        dst[:, cols] = (new * alive).astype(BF16)
        if save:
            learned[head, t - 7, :, cols] = new.astype(BF16)

    def step(t, src, dst, save, begin=False, ahead=True, between=None):
        multiply(src, 0, 6)
        if not begin:
            settle(t - 1, 3, src, save)
        multiply(src, 6, 20)
        if between is not None:
            between()
        settle(t, 0, dst, save)
        multiply(src, 20, 26)
        settle(t, 1, dst, save)
        multiply(src, 26, 32, ahead)
        settle(t, 2, dst, save)

    def route(kind, i, owner, to):
        ref = learned.at[head_of(owner), i + 1]
        return pltpu.make_async_remote_copy(
            src_ref=ref,
            dst_ref=ref,
            send_sem=route_send.at[kind, i],
            recv_sem=route_recv.at[kind, i],
            device_id=device(to),
            device_id_type=MESH,
        )

    def send_out(i):
        route(1, i, me, facing).start()
        route(0, i, me, other).start()

    def hand_on(i):
        route(1, i, me, facing).wait_recv()
        route(2, i, facing, other).start()

    def burn(i, _):
        step(2 * i, even, odd, False)
        step(2 * i + 1, odd, even, False)
        return 0

    lag = 6

    def learn(i, _):
        stage(0)
        for u in range(4):
            at = 4 * i + u

            def exchange():
                if u:
                    send_out(at - 1)
                else:

                    @pl.when(i > 0)
                    def _():
                        send_out(at - 1)

                @pl.when(at >= lag)
                def _():
                    hand_on(at - lag)

            src, dst = (odd, even) if u % 2 else (even, odd)
            step(at + 8, src, dst, True, ahead=u < 3, between=exchange)

        @pl.when(i < 3)
        def _():
            project(pl.multiple_of((4 * i + 12) * seqs, 128))

        return 0

    stage(0)
    step(0, even, odd, False, begin=True)
    step(1, odd, even, False)
    lax.fori_loop(1, 3, burn, 0)
    step(6, even, odd, False)
    step(7, odd, even, False, ahead=False)
    lax.fori_loop(0, 4, learn, 0)
    settle(23, 3, even, True)
    send_out(15)
    for unit in units:
        pltpu.matmul_pop(unit.spare)

    def pack(s, half):
        for n in range(4):
            unit, cols = units[n % 2], slice(256 * n, 256 * n + 256)
            rows = learned[s, 8 * half + 1 : 8 * half + 9, :, cols].reshape(256, 256)
            got = pltpu.matmul_pop(unit.run(unit.wide[2 * (s % 2) + n // 2], [(pick[s], rows)]))
            packed[:, (2 * s + half) * 16 : (2 * s + half) * 16 + 16, cols] = got.astype(BF16).reshape(8, 16, 256)

    for load in weights:
        load.wait()
    for i in range(16 - lag, 16):
        hand_on(i)
    for i in range(8):
        route(0, i, me, other).wait_recv()
        route(2, i, facing, other).wait_recv()
    for s in range(4):
        pack(s, 0)
    for i in range(8, 16):
        route(0, i, me, other).wait_recv()
        route(2, i, facing, other).wait_recv()
    for s in range(4):
        pack(s, 1)
    valid_lane = iota((128, 128), 1) < ACTIONS
    def inner(p):
        accs = []
        for n in range(4):
            unit, cols = units[n % 2], slice(256 * n, 256 * n + 256)
            pairs = [
                (packed[p, :, 256 * k : 256 * k + 256], hidden_w[p, 256 * k : 256 * k + 256, cols])
                for k in range(4)
            ]
            accs.append(unit.run(unit.wide[2 * (p % 2) + n // 2], pairs))
        return accs

    def outer(p, accs):
        mid = [jnp.maximum(pltpu.matmul_pop(acc), 0.0).astype(BF16) for acc in accs]
        nil = jnp.zeros((256, 128), BF16)
        pairs = []
        for k in range(4):
            part = slice(256 * (k % 2), 256 * (k % 2) + 256)
            if k < 2:
                tile = [value_w[p, part, :], nil]
            else:
                tile = [adv_w[p, part, :]] * 2
            pairs.append((mid[k], jnp.concatenate(tile, axis=1)))
        unit = units[p % 2]
        got = pltpu.matmul_pop(unit.run(unit.wide[4], pairs))
        mean = jnp.sum(got[:, 128:256], axis=1, keepdims=True) * (1.0 / ACTIONS)
        return jnp.where(valid_lane, got[:, 0:128] - mean, 0.0)

    ready = inner(0)
    for quad in range(2):
        total = None
        for j in range(4):
            p = 4 * quad + j
            now, ready = ready, inner(p + 1) if p < 7 else None
            q = outer(p, now)
            if j:
                q = pltpu.roll(q, 32 * j, 1)
            total = q if total is None else total + q
        for s in range(4):
            answers[s, 32 * quad : 32 * quad + 32, :] = total[32 * s : 32 * s + 32].astype(BF16)
    replies[head] = answers[head]
    back = []
    for to in (diagonal, facing, other):
        back.append(copies.send(answers.at[head_of(to)], replies.at[head], to))
    for copy in back:
        copy.wait_recv()
    got = replies[...].reshape(256, 128).astype(F32).T.astype(BF16)
    found = [
        pltpu.matmul_pop(unit.run(unit.wide[0], [(got, spread[:, 256 * n : 256 * n + 256])]))
        for n, unit in enumerate(units)
    ]
    found = jnp.concatenate(found, axis=1) * group[...]
    found = found[0:32] + found[32:64] + found[64:96] + found[96:128]
    chosen = jnp.where(iota((32, 512), 0).astype(F32) == act[0:1, :], found, 0.0)
    taken = jnp.sum(chosen, axis=0, keepdims=True)
    for t in range(16):
        tile, off = t // 4 * 128, t % 4 * 32
        now = found[0:24, tile : tile + 128]
        mine = jnp.broadcast_to(taken[:, tile : tile + 128], (8, 128))
        if off:
            now = pltpu.roll(now, 128 - off, 1)
            mine = pltpu.roll(mine, 128 - off, 1)
        q_out[pl.ds(t, ACTIONS, stride=16), :] = now[0:ACTIONS, 0:32]
        taken_out[t : t + 1, :] = mine[0:1, 0:32]
    for i in range(16):
        route(0, i, me, other).wait_send()
        route(1, i, me, facing).wait_send()
        route(2, i, facing, other).wait_send()
    for copy in copies.sent:
        copy.wait_send()


def shards(
    features,
    state_h,
    state_c,
    valid,
    ends,
    policy,
    actions,
    w_input,
    w_recur,
    lstm_bias,
    w_hidden,
    w_value,
    w_advantage,
):
    vmem = pl.BlockSpec(memory_space=pltpu.VMEM)
    held = [(16, 4, 256), (32, 4, 256), (24, 32), (16, 32), (1, 32), (1, 32), (4, 1024), (8, 512), (ACTIONS, 8, 512)]
    held += [(32, 1024), (32, 1024)]
    kinds = [BF16] * 2 + [jnp.int32] * 4 + [F32] + [BF16] * 4
    dma = pltpu.SemaphoreType.DMA
    given = (
        w_input,
        w_recur,
        ends.T,
        actions.T,
        policy.T,
        valid[None, :],
        lstm_bias,
        w_value,
        w_advantage.transpose(2, 0, 1),
        state_h,
        state_c,
        features.reshape(6, 128, features.shape[2]),
        w_hidden,
    )
    pinned = [pltpu.with_memory_space_constraint(v, pltpu.HBM) for v in given]
    q, taken = pl.pallas_call(
        core_kernel,
        out_shape=(
            jax.ShapeDtypeStruct((ACTIONS * 16, 32), F32),
            jax.ShapeDtypeStruct((16, 32), F32),
        ),
        in_specs=[pl.BlockSpec(memory_space=pltpu.HBM)] * 13,
        out_specs=(vmem, vmem),
        scratch_shapes=[pltpu.VMEM(shape, kind) for shape, kind in zip(held, kinds)]
        + [
            pltpu.VMEM((4, 48, 256), BF16),
            pltpu.VMEM((2, 4, 2, 2, 4, 4, 48, 256), BF16),
            pltpu.VMEM((16, 768, 256), F32),
            pltpu.VMEM((32, 1024), BF16),
            pltpu.VMEM((32, 1024), BF16),
            pltpu.VMEM((32, 1024), F32),
            pltpu.VMEM((25, 32, 128), F32),
            pltpu.VMEM((768, 512), BF16),
            pltpu.VMEM((8, 1024, 1024), BF16),
            pltpu.VMEM((4, 17, 32, 1024), BF16),
            pltpu.VMEM((8, 128, 1024), BF16),
            pltpu.VMEM((128, 128), F32),
            pltpu.VMEM((1024, 128), F32),
            pltpu.VMEM((4, 16, 256), F32),
            pltpu.VMEM((4, 128, 256), BF16),
            pltpu.VMEM((8, 512, 128), BF16),
            pltpu.VMEM((8, 512, 128), BF16),
            pltpu.VMEM((256, 512), BF16),
            pltpu.VMEM((128, 512), F32),
            pltpu.VMEM((8, 512), F32),
            pltpu.VMEM((4, 64, 128), BF16),
            pltpu.VMEM((4, 64, 128), BF16),
            dma((20,)),
            dma((SENDS,)),
            dma((SENDS,)),
            dma((3, 16)),
            dma((3, 16)),
        ],
        compiler_params=pltpu.CompilerParams(
            collective_id=0, has_side_effects=True, vmem_limit_bytes=int(53.5 * 2**20)
        ),
        name="core",
    )(*pinned)
    return q.reshape(ACTIONS, 16, 32).transpose(2, 1, 0), taken.T


def solution(mesh):
    return jax.shard_map(
        shards,
        mesh=mesh,
        in_specs=(
            P(("batch", "head"), None, None),
            P(("batch", "head"), None),
            P(("batch", "head"), None),
            P(("batch", "head")),
            P(("batch", "head"), None),
            P(("batch", "head"), None),
            P(("batch", "head"), None),
            P("batch", None, "head"),
            P("batch", None, "head"),
            P(),
            P("head", None, None),
            P("head", None),
            P("head", None, None),
        ),
        out_specs=(P(("batch", "head"), None, None), P(("batch", "head"), None)),
        check_vma=False,
    )
```

```python
import jax
import jax.numpy as jnp
from jax import lax
from jax.experimental import pallas as pl
from jax.experimental.pallas import tpu as pltpu
from jax.sharding import PartitionSpec as P

ACTIONS = 18
MESH = pl.DeviceIdType.MESH
ORDERS = ("xyz", "yzx", "zxy")
SENDS = 176
F32 = jnp.float32
BF16 = jnp.bfloat16


def here():
    b = lax.axis_index("batch")
    h = lax.axis_index("head")
    return {"x": b % 4, "y": b // 4 % 2 * 2 + h // 2, "z": b // 8, "c": h % 2}


def device(at):
    return (at["z"] * 8 + at["y"] // 2 * 4 + at["x"], at["y"] % 2 * 2 + at["c"])


def shifted(at, axis, by):
    return {**at, axis: (at[axis] + by + 4) % 4}


def greet(me):
    barrier = pltpu.get_barrier_semaphore()
    other = {**me, "c": 1 - me["c"]}
    peers = [shifted(me, a, d) for a in "xyz" for d in (1, -1, 2)]
    peers += [other, {**other, "y": me["y"] + 1 - 2 * (me["y"] % 2)}]
    for p in peers:
        pl.semaphore_signal(barrier, inc=1, device_id=device(p), device_id_type=MESH)
    return lambda: pl.semaphore_wait(barrier, len(peers))


class Copies:
    def __init__(self, send_sem, recv_sem):
        self.sems = (send_sem, recv_sem)
        self.sent = []

    def send(self, src, dst, to):
        k = len(self.sent)
        copy = pltpu.make_async_remote_copy(
            src_ref=src,
            dst_ref=dst,
            send_sem=self.sems[0].at[k],
            recv_sem=self.sems[1].at[k],
            device_id=device(to),
            device_id_type=MESH,
        )
        copy.start()
        self.sent.append(copy)
        return copy

    def push(self, ref, to):
        return self.send(ref, ref, to)


def gather(me, shard, full, copies, meanwhile, later):
    other = {**me, "c": 1 - me["c"]}
    crossed = {k: [] for k in range(3)}

    def region(part, at, free=None, half=None):
        z, x = at["z"], at["x"]
        y = (at["y"] // 2, at["y"] % 2)
        if free == "y":
            y = (slice(None) if half is None else half, slice(None))
        elif free is not None:
            span = slice(None) if half is None else pl.ds(2 * half, 2)
            z, x = (span, x) if free == "z" else (z, span)
        return full.at[me["c"], z, y[0], y[1], x, :, pl.ds(16 * part, 16), :]

    def cross(k, ref):
        crossed[k].append(copies.push(ref, other))

    def own(k):
        return shard.at[:, pl.ds(16 * k, 16), :]

    first, relay = {}, {}
    line = {(k, d): [] for k in range(3) for d in (1, -1)}
    third = {(k, m, d): [] for k in range(3) for m in range(4) for d in (1, -1)}
    for d in (1, -1, 2):
        for k, (a, b, c) in enumerate(ORDERS):
            first[k, d] = copies.send(own(k), region(k, me), shifted(me, a, d))

    def along_both(k, at, src):
        a, b, c = ORDERS[k]
        for d in (1, -1):
            line[k, d].append(copies.send(src, region(k, at), shifted(me, b, d)))
        for d in (1, -1):
            third[k, 0, d].append(copies.send(src, region(k, at), shifted(me, c, d)))

    def along_last(k, m, at):
        a, b, c = ORDERS[k]
        for d in (1, -1):
            third[k, m, d].append(copies.push(region(k, at, free=a), shifted(me, c, d)))

    for k in range(3):
        along_both(k, me, own(k))
    full[me["c"], me["z"], me["y"] // 2, me["y"] % 2, me["x"]] = shard[...]
    meanwhile()
    for d in (1, -1, 2):
        for k, (a, b, c) in enumerate(ORDERS):
            first[k, d].wait_recv()
            at = shifted(me, a, -d)
            along_both(k, at, region(k, at))
    for k, (a, b, c) in enumerate(ORDERS):
        cross(k, region(k, me, free=a))
    for k, (a, b, c) in enumerate(ORDERS):
        for m, d in ((1, 1), (2, -1)):
            for copy in line[k, d]:
                copy.wait_recv()
            at = shifted(me, b, -d)
            relay[k, d] = copies.push(region(k, at, free=a, half=(1 - d) // 2), shifted(me, b, d))
            along_last(k, m, at)
            cross(k, region(k, at, free=a))
    for k, (a, b, c) in enumerate(ORDERS):
        for d in (1, -1):
            relay[k, d].wait_recv()
        at = shifted(me, b, 2)
        along_last(k, 3, at)
        cross(k, region(k, at, free=a))
    later()
    relay = {}
    offsets = (0, -1, 1, 2)
    for m in range(4):
        for k, (a, b, c) in enumerate(ORDERS):
            for d in (1, -1):
                for copy in third[k, m, d]:
                    copy.wait_recv()
                at = shifted(shifted(me, b, offsets[m]), c, -d)
                relay[k, m, d] = copies.push(region(k, at, free=a, half=(1 - d) // 2), shifted(me, c, d))
                cross(k, region(k, at, free=a))
    for m in range(4):
        for k, (a, b, c) in enumerate(ORDERS):
            for d in (1, -1):
                relay[k, m, d].wait_recv()
            cross(k, region(k, shifted(shifted(me, b, offsets[m]), c, 2), free=a))

    def crossing(k):
        for copy in crossed[k]:
            copy.wait_recv()

    return crossing


def sigmoid(v):
    return 0.5 * jnp.tanh(0.5 * v) + 0.5


def iota(shape, dim):
    return lax.broadcasted_iota(jnp.int32, shape, dim)


def ones_where(mask, dtype):
    return jnp.where(mask, 1.0, 0.0).astype(dtype)


def prepare(ends, actions, policy, valid, small, wv, wa, wide, head, keep, info, value_w, adv_w, spread, group):
    small[...] = jnp.zeros((128, 128), F32)
    small[0:24, 0:32] = ends[...].astype(F32)
    small[24:40, 0:32] = actions[...].astype(F32)
    small[40:41, 0:32] = policy[...].astype(F32)
    small[41:42, 0:32] = valid[...].astype(F32)
    by_seq = small[...].T
    for t in range(24):
        keep[t] = jnp.broadcast_to(1.0 - by_seq[0:32, t : t + 1], (32, 128))
    keep[24] = jnp.ones((32, 128), F32)

    def tiled():
        rows = small[24:48, :]
        return rows + pltpu.roll(rows, 32, 1) + pltpu.roll(rows, 64, 1) + pltpu.roll(rows, 96, 1)

    across = tiled()[16:17, :]
    same = jnp.broadcast_to(by_seq[0:32, 40:41], (32, 128)) == across
    earlier = iota((32, 128), 0) < (iota((32, 128), 1) & 31)
    rank = jnp.sum(ones_where(same & earlier, F32), axis=0, keepdims=True)
    info[head] = jnp.concatenate(
        [jnp.broadcast_to(jnp.concatenate([v, v], axis=1), (8, 256)) for v in (across, rank)], axis=0
    )
    start = jnp.broadcast_to(by_seq[0:32, 41:42], (32, 128)) * keep[0]

    def finish():
        rows, across, rank = tiled(), info[head, 0:1, 0:128], info[head, 8:9, 0:128]
        lane = iota((1, 512), 1)
        step = lane >> 5
        number = jnp.concatenate([across] * 4, axis=1).astype(jnp.int32)
        slot = (number >> 2) * 32 + (step >> 3) * 16 + (step & 7)
        slot = slot + jnp.concatenate([rank] * 4, axis=1).astype(jnp.int32) * 8
        spread[...] = ones_where(iota((256, 512), 0) == slot, BF16)
        group[...] = ones_where((iota((128, 512), 0) >> 5) == (number & 3), F32)
        picks = jnp.concatenate([rows[0:16, :]] * 4, axis=1)
        on = iota((16, 512), 0) == (iota((16, 512), 1) >> 5)
        for p in range(8):
            line = wv[p : p + 1, :].astype(F32)
            value_w[p] = jnp.broadcast_to(line, (128, 512)).T.astype(BF16)
        wide[...] = jnp.zeros((1024, 128), F32)
        for a in range(ACTIONS):
            line = wa[a].astype(F32)
            for col in range(4):
                wide[pl.ds(256 * col + a, 8, stride=32), :] = line[:, 128 * col : 128 * col + 128]
        for p in range(8):
            part = [wide[256 * col + 32 * p : 256 * col + 32 * p + 32, :] for col in range(4)]
            part = jnp.concatenate([jnp.concatenate(part, axis=1), jnp.zeros((96, 512), F32)], axis=0)
            adv_w[p] = part.T.astype(BF16)
        return jnp.sum(jnp.where(on, picks, 0.0), axis=0, keepdims=True)

    return start, finish


class Unit:
    def __init__(self, number, accs):
        self.number = number
        self.gates, self.spare, self.wide = accs
        self.turn = 0

    def push(self, tile, slot):
        pltpu.matmul_push_rhs(tile, staging_register=slot, mxu_index=self.number)

    def run(self, acc, pairs):
        for rows, tile in pairs:
            self.push(tile, self.turn)
            pltpu.matmul_acc_lhs(acc, rows, load_staged_rhs=self.turn)
            self.turn = 1 - self.turn
        return acc


def accumulators(number):
    acc = pltpu.ACC(number)
    return (
        [acc((32, 256), F32) for _ in range(8)],
        acc((96, 256), F32),
        [acc((128, 256), F32) for _ in range(5)],
    )


def core_kernel(*refs):
    pl.run_scoped(lambda first, second: core(refs, (Unit(0, first), Unit(1, second))), accumulators(0), accumulators(1))


def core(refs, units):
    given, (q_out, taken_out), held = refs[:13], refs[13:15], refs[15:26]
    w_in, w_rec, ends, actions, policy, valid, bias, wv, wa, state_h, state_c = held
    (
        shard, full, pre, even, odd, cell, keep, feat, hidden_w, learned, packed, small, wide, info, pick,
        value_w, adv_w, spread, group, act, answers, replies, local_sem, send_sem, recv_sem, route_send, route_recv,
    ) = refs[26:]
    wh_hbm = given[12]
    me = here()
    met = greet(me)
    for unit in units:
        for acc in unit.gates + [unit.spare] + unit.wide:
            pltpu.matmul_pop(acc)
    seqs = 32
    head = me["y"] % 2 * 2 + me["c"]
    other = {**me, "c": 1 - me["c"]}
    facing = {**me, "y": me["y"] + 1 - 2 * (me["y"] % 2)}
    diagonal = {**facing, "c": 1 - me["c"]}
    head_of = lambda at: at["y"] % 2 * 2 + at["c"]
    raw = packed.at[0:6, :, 0:512]
    loads = [pltpu.make_async_copy(given[k], ref, local_sem.at[8 + k]) for k, ref in enumerate(held + (raw,))]
    for load in loads:
        load.start()
    for load in loads[0:2]:
        load.wait()
    for g in range(4):
        shard[g, 0:16, :] = w_in[:, g, :]
        shard[g, 16:48, :] = w_rec[:, g, :]
    met()
    copies = Copies(send_sem, recv_sem)
    told = []
    rest = []
    weights = [pltpu.make_async_copy(wh_hbm.at[p], hidden_w.at[p], local_sem.at[p]) for p in range(8)]

    def meanwhile():
        for load in loads[2:]:
            load.wait()
        start, finish = prepare(
            ends, actions, policy, valid, small, wv, wa, wide, head, keep, info, value_w, adv_w, spread, group
        )
        rest.append(finish)
        start = jnp.concatenate([start] * 8, axis=1)
        even[...] = (state_h[...].astype(F32) * start).astype(BF16)
        cell[...] = state_c[...].astype(F32) * start
        for to in (other, facing, diagonal):
            told.append(copies.push(info.at[head], to))
        for load in weights:
            load.start()

    def later():
        act[...] = jnp.broadcast_to(rest[0](), (8, 512))
        for part in range(6):
            row = iota((128, 768), 0)
            order = ones_where(iota((128, 768), 1) == (row & 31) * 24 + (row >> 5) + 4 * part, BF16)
            for n, unit in enumerate(units):
                cols = slice(256 * n, 256 * n + 256)
                pairs = [
                    (order[:, 256 * k : 256 * k + 256], packed[2 * k : 2 * k + 2, :, cols].reshape(256, 256))
                    for k in range(3)
                ]
                got = pltpu.matmul_pop(unit.run(unit.wide[part % 4], pairs))
                feat[128 * part : 128 * part + 128, cols] = got.astype(BF16)

    crossing = gather(me, shard, full, copies, meanwhile, later)
    for copy in told:
        copy.wait_recv()
    lane = iota((128, 256), 1)
    row = iota((128, 256), 0)
    step_at = (lane >> 5) == (row & 7)
    for s in range(4):
        mine = info[s, 0:1, :] == ((row >> 4) + 8 * head).astype(F32)
        cap = info[s, 8:9, :] == ((row >> 3) & 1).astype(F32)
        pick[s] = ones_where(mine & cap & step_at, BF16)

    def project(start):
        rows = pl.ds(start, 128)
        f = [feat[rows, 256 * k : 256 * k + 256] for k in range(2)]
        for n in range(16):
            hp, g = n // 4, n % 4
            unit = units[n % 2]
            pairs = [
                (f[k], full[hp % 2, 2 * k : 2 * k + 2, :, hp // 2, :, g, 0:16, :].reshape(256, 256))
                for k in range(2)
            ]
            got = pltpu.matmul_pop(unit.run(unit.wide[n // 2 % 4], pairs))
            pre[n, rows, :] = got + bias[g : g + 1, hp * 256 : hp * 256 + 256]

    crossing(0)
    for part in range(3):
        project(128 * part)
    crossing(1)
    crossing(2)

    tiles = [(hp, pair, 0) for hp in range(4) for pair in range(2)]
    tiles += [(hp, pair, k) for hp in range(4) for k in range(1, 4) for pair in range(2)]

    def stage(i):
        hp, pair, k = tiles[i % 32]
        for q, unit in enumerate(units):
            w = full[hp % 2, k, :, hp // 2, :, 2 * pair + q, 16:48, :].reshape(256, 256)
            unit.push(w, i % 2)

    def multiply(src, first, last, ahead=True):
        for i in range(first, last):
            if ahead or i + 1 < last:
                stage(i + 1)
            hp, pair, k = tiles[i]
            h = src[:, 256 * k : 256 * k + 256]
            for unit in units:
                pltpu.matmul_acc_lhs(unit.gates[2 * hp + pair], h, load_staged_rhs=i % 2)
            h = jnp.concatenate([h, h, h], axis=0)
            for unit in units:
                pltpu.matmul_acc_lhs(unit.spare, h)

    def settle(t, hp, dst, save):
        rows = pl.ds(pl.multiple_of(t * seqs, seqs), seqs)
        alive = keep[t + 1]
        alive = jnp.concatenate([alive, alive], axis=1)
        gate = [pltpu.matmul_pop(units[g % 2].gates[2 * hp + g // 2]) for g in range(4)]
        gate = [gate[g] + pre[hp * 4 + g, rows, :] for g in range(4)]
        cols = slice(hp * 256, hp * 256 + 256)
        c = sigmoid(gate[1]) * cell[:, cols] + sigmoid(gate[0]) * jnp.tanh(gate[2])
        new = sigmoid(gate[3]) * jnp.tanh(c)
        cell[:, cols] = c * alive
        dst[:, cols] = (new * alive).astype(BF16)
        if save:
            learned[head, t - 7, :, cols] = new.astype(BF16)

    def step(t, src, dst, save, begin=False, ahead=True, between=None):
        multiply(src, 0, 6)
        if not begin:
            settle(t - 1, 3, src, save)
        multiply(src, 6, 12)
        if between is not None:
            between()
        multiply(src, 12, 20)
        settle(t, 0, dst, save)
        multiply(src, 20, 26)
        settle(t, 1, dst, save)
        multiply(src, 26, 32, ahead)
        settle(t, 2, dst, save)

    def route(kind, i, owner, to):
        ref = learned.at[head_of(owner), i + 1]
        return pltpu.make_async_remote_copy(
            src_ref=ref,
            dst_ref=ref,
            send_sem=route_send.at[kind, i],
            recv_sem=route_recv.at[kind, i],
            device_id=device(to),
            device_id_type=MESH,
        )

    def send_out(i):
        route(1, i, me, facing).start()
        route(0, i, me, other).start()

    def hand_on(i):
        route(1, i, me, facing).wait_recv()
        route(2, i, facing, other).start()

    def burn(i, _):
        step(2 * i, even, odd, False)
        step(2 * i + 1, odd, even, False)
        return 0

    lag = 6

    def learn(i, _):
        stage(0)
        for u in range(4):
            at = 4 * i + u

            def exchange():
                if u:
                    send_out(at - 1)
                else:

                    @pl.when(i > 0)
                    def _():
                        send_out(at - 1)

                @pl.when(at >= lag)
                def _():
                    hand_on(at - lag)

            src, dst = (odd, even) if u % 2 else (even, odd)
            step(at + 8, src, dst, True, ahead=u < 3, between=exchange)

        @pl.when(i < 3)
        def _():
            project(pl.multiple_of((4 * i + 12) * seqs, 128))

        return 0

    stage(0)
    step(0, even, odd, False, begin=True)
    step(1, odd, even, False)
    lax.fori_loop(1, 3, burn, 0)
    step(6, even, odd, False)
    step(7, odd, even, False, ahead=False)
    lax.fori_loop(0, 4, learn, 0)
    settle(23, 3, even, True)
    send_out(15)
    for unit in units:
        pltpu.matmul_pop(unit.spare)

    def pack(turn, s, half):
        at = pl.ds(pl.multiple_of((2 * s + half) * 16, 16), 16)
        for n in range(4):
            unit, cols = units[n % 2], slice(256 * n, 256 * n + 256)
            rows = learned[s, 8 * half + 1 : 8 * half + 9, :, cols].reshape(256, 256)
            got = pltpu.matmul_pop(unit.run(unit.wide[2 * turn + n // 2], [(pick[s], rows)]))
            packed[:, at, cols] = got.astype(BF16).reshape(8, 16, 256)

    for i in range(16 - lag, 13):
        hand_on(i)
    for load in weights:
        load.wait()
    for i in range(16):
        route(0, i, me, other).wait_recv()
    for half in range(2):
        pack(0, head_of(me), half)
        pack(1, head_of(other), half)
    for i in range(13, 16):
        hand_on(i)
    for half in range(2):
        for i in range(8 * half, 8 * half + 8):
            route(2, i, facing, other).wait_recv()
        pack(0, head_of(facing), half)
        pack(1, head_of(diagonal), half)
    valid_lane = iota((128, 128), 1) < ACTIONS
    def inner(p):
        accs = []
        for n in range(4):
            unit, cols = units[n % 2], slice(256 * n, 256 * n + 256)
            pairs = [
                (packed[p, :, 256 * k : 256 * k + 256], hidden_w[p, 256 * k : 256 * k + 256, cols])
                for k in range(4)
            ]
            accs.append(unit.run(unit.wide[2 * (p % 2) + n // 2], pairs))
        return accs

    def outer(p, accs):
        mid = [jnp.maximum(pltpu.matmul_pop(acc), 0.0).astype(BF16) for acc in accs]
        nil = jnp.zeros((256, 128), BF16)
        pairs = []
        for k in range(4):
            part = slice(256 * (k % 2), 256 * (k % 2) + 256)
            if k < 2:
                tile = [value_w[p, part, :], nil]
            else:
                tile = [adv_w[p, part, :]] * 2
            pairs.append((mid[k], jnp.concatenate(tile, axis=1)))
        unit = units[p % 2]
        got = pltpu.matmul_pop(unit.run(unit.wide[4], pairs))
        mean = jnp.sum(got[:, 128:256], axis=1, keepdims=True) * (1.0 / ACTIONS)
        return jnp.where(valid_lane, got[:, 0:128] - mean, 0.0)

    ready = inner(0)
    for quad in range(2):
        total = None
        for j in range(4):
            p = 4 * quad + j
            now, ready = ready, inner(p + 1) if p < 7 else None
            q = outer(p, now)
            if j:
                q = pltpu.roll(q, 32 * j, 1)
            total = q if total is None else total + q
        for s in range(4):
            answers[s, 32 * quad : 32 * quad + 32, :] = total[32 * s : 32 * s + 32].astype(BF16)
    replies[head] = answers[head]
    back = []
    for to in (diagonal, facing, other):
        back.append(copies.send(answers.at[head_of(to)], replies.at[head], to))
    for copy in back:
        copy.wait_recv()
    got = replies[...].reshape(256, 128).astype(F32).T.astype(BF16)
    found = [
        pltpu.matmul_pop(unit.run(unit.wide[0], [(got, spread[:, 256 * n : 256 * n + 256])]))
        for n, unit in enumerate(units)
    ]
    found = jnp.concatenate(found, axis=1) * group[...]
    found = found[0:32] + found[32:64] + found[64:96] + found[96:128]
    chosen = jnp.where(iota((32, 512), 0).astype(F32) == act[0:1, :], found, 0.0)
    taken = jnp.sum(chosen, axis=0, keepdims=True)
    for t in range(16):
        tile, off = t // 4 * 128, t % 4 * 32
        now = found[0:24, tile : tile + 128]
        mine = jnp.broadcast_to(taken[:, tile : tile + 128], (8, 128))
        if off:
            now = pltpu.roll(now, 128 - off, 1)
            mine = pltpu.roll(mine, 128 - off, 1)
        q_out[pl.ds(t, ACTIONS, stride=16), :] = now[0:ACTIONS, 0:32]
        taken_out[t : t + 1, :] = mine[0:1, 0:32]
    for i in range(16):
        route(0, i, me, other).wait_send()
        route(1, i, me, facing).wait_send()
        route(2, i, facing, other).wait_send()
    for copy in copies.sent:
        copy.wait_send()


def shards(
    features,
    state_h,
    state_c,
    valid,
    ends,
    policy,
    actions,
    w_input,
    w_recur,
    lstm_bias,
    w_hidden,
    w_value,
    w_advantage,
):
    vmem = pl.BlockSpec(memory_space=pltpu.VMEM)
    held = [(16, 4, 256), (32, 4, 256), (24, 32), (16, 32), (1, 32), (1, 32), (4, 1024), (8, 512), (ACTIONS, 8, 512)]
    held += [(32, 1024), (32, 1024)]
    kinds = [BF16] * 2 + [jnp.int32] * 4 + [F32] + [BF16] * 4
    dma = pltpu.SemaphoreType.DMA
    given = (
        w_input,
        w_recur,
        ends.T,
        actions.T,
        policy.T,
        valid[None, :],
        lstm_bias,
        w_value,
        w_advantage.transpose(2, 0, 1),
        state_h,
        state_c,
        features.reshape(6, 128, features.shape[2]),
        w_hidden,
    )
    pinned = [pltpu.with_memory_space_constraint(v, pltpu.HBM) for v in given]
    q, taken = pl.pallas_call(
        core_kernel,
        out_shape=(
            jax.ShapeDtypeStruct((ACTIONS * 16, 32), F32),
            jax.ShapeDtypeStruct((16, 32), F32),
        ),
        in_specs=[pl.BlockSpec(memory_space=pltpu.HBM)] * 13,
        out_specs=(vmem, vmem),
        scratch_shapes=[pltpu.VMEM(shape, kind) for shape, kind in zip(held, kinds)]
        + [
            pltpu.VMEM((4, 48, 256), BF16),
            pltpu.VMEM((2, 4, 2, 2, 4, 4, 48, 256), BF16),
            pltpu.VMEM((16, 768, 256), F32),
            pltpu.VMEM((32, 1024), BF16),
            pltpu.VMEM((32, 1024), BF16),
            pltpu.VMEM((32, 1024), F32),
            pltpu.VMEM((25, 32, 128), F32),
            pltpu.VMEM((768, 512), BF16),
            pltpu.VMEM((8, 1024, 1024), BF16),
            pltpu.VMEM((4, 17, 32, 1024), BF16),
            pltpu.VMEM((8, 128, 1024), BF16),
            pltpu.VMEM((128, 128), F32),
            pltpu.VMEM((1024, 128), F32),
            pltpu.VMEM((4, 16, 256), F32),
            pltpu.VMEM((4, 128, 256), BF16),
            pltpu.VMEM((8, 512, 128), BF16),
            pltpu.VMEM((8, 512, 128), BF16),
            pltpu.VMEM((256, 512), BF16),
            pltpu.VMEM((128, 512), F32),
            pltpu.VMEM((8, 512), F32),
            pltpu.VMEM((4, 64, 128), BF16),
            pltpu.VMEM((4, 64, 128), BF16),
            dma((20,)),
            dma((SENDS,)),
            dma((SENDS,)),
            dma((3, 16)),
            dma((3, 16)),
        ],
        compiler_params=pltpu.CompilerParams(
            collective_id=0, has_side_effects=True, vmem_limit_bytes=int(53.5 * 2**20)
        ),
        name="core",
    )(*pinned)
    return q.reshape(ACTIONS, 16, 32).transpose(2, 1, 0), taken.T


def solution(mesh):
    return jax.shard_map(
        shards,
        mesh=mesh,
        in_specs=(
            P(("batch", "head"), None, None),
            P(("batch", "head"), None),
            P(("batch", "head"), None),
            P(("batch", "head")),
            P(("batch", "head"), None),
            P(("batch", "head"), None),
            P(("batch", "head"), None),
            P("batch", None, "head"),
            P("batch", None, "head"),
            P(),
            P("head", None, None),
            P("head", None),
            P("head", None, None),
        ),
        out_specs=(P(("batch", "head"), None, None), P(("batch", "head"), None)),
        check_vma=False,
    )
```

```python
import jax
import jax.numpy as jnp
from jax import lax
from jax.experimental import pallas as pl
from jax.experimental.pallas import tpu as pltpu
from jax.sharding import PartitionSpec as P

ACTIONS = 18
MESH = pl.DeviceIdType.MESH
ORDERS = ("xyz", "yzx", "zxy")
SENDS = 176
F32 = jnp.float32
BF16 = jnp.bfloat16


def here():
    b = lax.axis_index("batch")
    h = lax.axis_index("head")
    return {"x": b % 4, "y": b // 4 % 2 * 2 + h // 2, "z": b // 8, "c": h % 2}


def device(at):
    return (at["z"] * 8 + at["y"] // 2 * 4 + at["x"], at["y"] % 2 * 2 + at["c"])


def shifted(at, axis, by):
    return {**at, axis: (at[axis] + by + 4) % 4}


def greet(me):
    barrier = pltpu.get_barrier_semaphore()
    other = {**me, "c": 1 - me["c"]}
    peers = [shifted(me, a, d) for a in "xyz" for d in (1, -1, 2)]
    peers += [other, {**other, "y": me["y"] + 1 - 2 * (me["y"] % 2)}]
    for p in peers:
        pl.semaphore_signal(barrier, inc=1, device_id=device(p), device_id_type=MESH)
    return lambda: pl.semaphore_wait(barrier, len(peers))


class Copies:
    def __init__(self, send_sem, recv_sem):
        self.sems = (send_sem, recv_sem)
        self.sent = []

    def send(self, src, dst, to):
        k = len(self.sent)
        copy = pltpu.make_async_remote_copy(
            src_ref=src,
            dst_ref=dst,
            send_sem=self.sems[0].at[k],
            recv_sem=self.sems[1].at[k],
            device_id=device(to),
            device_id_type=MESH,
        )
        copy.start()
        self.sent.append(copy)
        return copy

    def push(self, ref, to):
        return self.send(ref, ref, to)


def gather(me, shard, full, copies, meanwhile, later):
    other = {**me, "c": 1 - me["c"]}
    crossed = {k: [] for k in range(3)}

    def region(part, at, free=None, half=None, gates=slice(None)):
        z, x = at["z"], at["x"]
        y = (at["y"] // 2, at["y"] % 2)
        if free == "y":
            y = (slice(None) if half is None else half, slice(None))
        elif free is not None:
            span = slice(None) if half is None else pl.ds(2 * half, 2)
            z, x = (span, x) if free == "z" else (z, span)
        return full.at[me["c"], z, y[0], y[1], x, gates, pl.ds(16 * part, 16), :]

    def cross(k, ref):
        crossed[k].append(copies.push(ref, other))

    def own(k):
        return shard.at[:, pl.ds(16 * k, 16), :]

    first, relay = {}, {}
    line = {(k, d): [] for k in range(3) for d in (1, -1)}
    third = {(k, m, d): [] for k in range(3) for m in range(4) for d in (1, -1)}
    for d in (1, -1, 2):
        for k, (a, b, c) in enumerate(ORDERS):
            first[k, d] = copies.send(own(k), region(k, me), shifted(me, a, d))

    def along_both(k, at, src):
        a, b, c = ORDERS[k]
        for d in (1, -1):
            line[k, d].append(copies.send(src, region(k, at), shifted(me, b, d)))
        for d in (1, -1):
            third[k, 0, d].append(copies.send(src, region(k, at), shifted(me, c, d)))

    def along_last(k, m, at):
        a, b, c = ORDERS[k]
        for d in (1, -1):
            third[k, m, d].append(copies.push(region(k, at, free=a), shifted(me, c, d)))

    for k in range(3):
        along_both(k, me, own(k))
    full[me["c"], me["z"], me["y"] // 2, me["y"] % 2, me["x"]] = shard[...]
    meanwhile()
    for d in (1, -1, 2):
        for k, (a, b, c) in enumerate(ORDERS):
            first[k, d].wait_recv()
            at = shifted(me, a, -d)
            along_both(k, at, region(k, at))
    for k, (a, b, c) in enumerate(ORDERS):
        cross(k, region(k, me, free=a))
    for k, (a, b, c) in enumerate(ORDERS):
        for m, d in ((1, 1), (2, -1)):
            for copy in line[k, d]:
                copy.wait_recv()
            at = shifted(me, b, -d)
            relay[k, d] = copies.push(region(k, at, free=a, half=(1 - d) // 2), shifted(me, b, d))
            along_last(k, m, at)
            cross(k, region(k, at, free=a))
    for k, (a, b, c) in enumerate(ORDERS):
        for d in (1, -1):
            relay[k, d].wait_recv()
        at = shifted(me, b, 2)
        along_last(k, 3, at)
        cross(k, region(k, at, free=a))
    later()
    relay = {}
    offsets = (0, -1, 1, 2)
    for m in range(4):
        for k, (a, b, c) in enumerate(ORDERS):
            for d in (1, -1):
                for copy in third[k, m, d]:
                    copy.wait_recv()
                at = shifted(shifted(me, b, offsets[m]), c, -d)
                pair = pl.ds(1 - d, 2)
                relay[k, m, d] = copies.push(region(k, at, free=a, gates=pair), shifted(me, c, d))
                cross(k, region(k, at, free=a))
    for m in range(4):
        for k, (a, b, c) in enumerate(ORDERS):
            for d in (1, -1):
                relay[k, m, d].wait_recv()
            cross(k, region(k, shifted(shifted(me, b, offsets[m]), c, 2), free=a))

    def crossing(k):
        for copy in crossed[k]:
            copy.wait_recv()

    return crossing


def sigmoid(v):
    return 0.5 * jnp.tanh(0.5 * v) + 0.5


def iota(shape, dim):
    return lax.broadcasted_iota(jnp.int32, shape, dim)


def ones_where(mask, dtype):
    return jnp.where(mask, 1.0, 0.0).astype(dtype)


def prepare(ends, actions, policy, valid, small, wv, wa, wide, head, keep, info, value_w, adv_w, spread, group):
    small[...] = jnp.zeros((128, 128), F32)
    small[0:24, 0:32] = ends[...].astype(F32)
    small[24:40, 0:32] = actions[...].astype(F32)
    small[40:41, 0:32] = policy[...].astype(F32)
    small[41:42, 0:32] = valid[...].astype(F32)
    by_seq = small[...].T
    for t in range(24):
        keep[t] = jnp.broadcast_to(1.0 - by_seq[0:32, t : t + 1], (32, 128))
    keep[24] = jnp.ones((32, 128), F32)

    def tiled():
        rows = small[24:48, :]
        return rows + pltpu.roll(rows, 32, 1) + pltpu.roll(rows, 64, 1) + pltpu.roll(rows, 96, 1)

    across = tiled()[16:17, :]
    same = jnp.broadcast_to(by_seq[0:32, 40:41], (32, 128)) == across
    earlier = iota((32, 128), 0) < (iota((32, 128), 1) & 31)
    rank = jnp.sum(ones_where(same & earlier, F32), axis=0, keepdims=True)
    info[head] = jnp.concatenate(
        [jnp.broadcast_to(jnp.concatenate([v, v], axis=1), (8, 256)) for v in (across, rank)], axis=0
    )
    start = jnp.broadcast_to(by_seq[0:32, 41:42], (32, 128)) * keep[0]

    def finish():
        rows, across, rank = tiled(), info[head, 0:1, 0:128], info[head, 8:9, 0:128]
        lane = iota((1, 512), 1)
        step = lane >> 5
        number = jnp.concatenate([across] * 4, axis=1).astype(jnp.int32)
        slot = (number >> 2) * 32 + (step >> 3) * 16 + (step & 7)
        slot = slot + jnp.concatenate([rank] * 4, axis=1).astype(jnp.int32) * 8
        spread[...] = ones_where(iota((256, 512), 0) == slot, BF16)
        group[...] = ones_where((iota((128, 512), 0) >> 5) == (number & 3), F32)
        picks = jnp.concatenate([rows[0:16, :]] * 4, axis=1)
        on = iota((16, 512), 0) == (iota((16, 512), 1) >> 5)
        for p in range(8):
            line = wv[p : p + 1, :].astype(F32)
            value_w[p] = jnp.broadcast_to(line, (128, 512)).T.astype(BF16)
        wide[...] = jnp.zeros((1024, 128), F32)
        for a in range(ACTIONS):
            line = wa[a].astype(F32)
            for col in range(4):
                wide[pl.ds(256 * col + a, 8, stride=32), :] = line[:, 128 * col : 128 * col + 128]
        for p in range(8):
            part = [wide[256 * col + 32 * p : 256 * col + 32 * p + 32, :] for col in range(4)]
            part = jnp.concatenate([jnp.concatenate(part, axis=1), jnp.zeros((96, 512), F32)], axis=0)
            adv_w[p] = part.T.astype(BF16)
        return jnp.sum(jnp.where(on, picks, 0.0), axis=0, keepdims=True)

    return start, finish


class Unit:
    def __init__(self, number, accs):
        self.number = number
        self.gates, self.spare, self.wide = accs
        self.turn = 0

    def push(self, tile, slot):
        pltpu.matmul_push_rhs(tile, staging_register=slot, mxu_index=self.number)

    def run(self, acc, pairs):
        for rows, tile in pairs:
            self.push(tile, self.turn)
            pltpu.matmul_acc_lhs(acc, rows, load_staged_rhs=self.turn)
            self.turn = 1 - self.turn
        return acc


def accumulators(number):
    acc = pltpu.ACC(number)
    return (
        [acc((32, 256), F32) for _ in range(8)],
        acc((96, 256), F32),
        [acc((128, 256), F32) for _ in range(5)],
    )


def core_kernel(*refs):
    pl.run_scoped(lambda first, second: core(refs, (Unit(0, first), Unit(1, second))), accumulators(0), accumulators(1))


def core(refs, units):
    given, (q_out, taken_out), held = refs[:13], refs[13:15], refs[15:26]
    w_in, w_rec, ends, actions, policy, valid, bias, wv, wa, state_h, state_c = held
    (
        shard, full, pre, even, odd, cell, keep, feat, hidden_w, learned, packed, small, wide, info, pick,
        value_w, adv_w, spread, group, act, answers, replies, local_sem, send_sem, recv_sem, route_send, route_recv,
    ) = refs[26:]
    wh_hbm = given[12]
    me = here()
    met = greet(me)
    for unit in units:
        for acc in unit.gates + [unit.spare] + unit.wide:
            pltpu.matmul_pop(acc)
    seqs = 32
    head = me["y"] % 2 * 2 + me["c"]
    other = {**me, "c": 1 - me["c"]}
    facing = {**me, "y": me["y"] + 1 - 2 * (me["y"] % 2)}
    diagonal = {**facing, "c": 1 - me["c"]}
    head_of = lambda at: at["y"] % 2 * 2 + at["c"]
    raw = packed.at[0:6, :, 0:512]
    loads = [pltpu.make_async_copy(given[k], ref, local_sem.at[8 + k]) for k, ref in enumerate(held + (raw,))]
    for load in loads:
        load.start()
    for load in loads[0:2]:
        load.wait()
    for g in range(4):
        shard[g, 0:16, :] = w_in[:, g, :]
        shard[g, 16:48, :] = w_rec[:, g, :]
    met()
    copies = Copies(send_sem, recv_sem)
    told = []
    rest = []
    weights = [pltpu.make_async_copy(wh_hbm.at[p], hidden_w.at[p], local_sem.at[p]) for p in range(8)]

    def meanwhile():
        for load in loads[2:]:
            load.wait()
        start, finish = prepare(
            ends, actions, policy, valid, small, wv, wa, wide, head, keep, info, value_w, adv_w, spread, group
        )
        rest.append(finish)
        start = jnp.concatenate([start] * 8, axis=1)
        even[...] = (state_h[...].astype(F32) * start).astype(BF16)
        cell[...] = state_c[...].astype(F32) * start
        for to in (other, facing, diagonal):
            told.append(copies.push(info.at[head], to))
        for load in weights:
            load.start()

    def later():
        act[...] = jnp.broadcast_to(rest[0](), (8, 512))
        for part in range(6):
            row = iota((128, 768), 0)
            order = ones_where(iota((128, 768), 1) == (row & 31) * 24 + (row >> 5) + 4 * part, BF16)
            for n, unit in enumerate(units):
                cols = slice(256 * n, 256 * n + 256)
                pairs = [
                    (order[:, 256 * k : 256 * k + 256], packed[2 * k : 2 * k + 2, :, cols].reshape(256, 256))
                    for k in range(3)
                ]
                got = pltpu.matmul_pop(unit.run(unit.wide[part % 4], pairs))
                feat[128 * part : 128 * part + 128, cols] = got.astype(BF16)

    crossing = gather(me, shard, full, copies, meanwhile, later)
    for copy in told:
        copy.wait_recv()
    lane = iota((128, 256), 1)
    row = iota((128, 256), 0)
    step_at = (lane >> 5) == (row & 7)
    for s in range(4):
        mine = info[s, 0:1, :] == ((row >> 4) + 8 * head).astype(F32)
        cap = info[s, 8:9, :] == ((row >> 3) & 1).astype(F32)
        pick[s] = ones_where(mine & cap & step_at, BF16)

    def project(start):
        rows = pl.ds(start, 128)
        f = [feat[rows, 256 * k : 256 * k + 256] for k in range(2)]
        for n in range(16):
            hp, g = n // 4, n % 4
            unit = units[n % 2]
            pairs = [
                (f[k], full[hp % 2, 2 * k : 2 * k + 2, :, hp // 2, :, g, 0:16, :].reshape(256, 256))
                for k in range(2)
            ]
            got = pltpu.matmul_pop(unit.run(unit.wide[n // 2 % 4], pairs))
            pre[n, rows, :] = got + bias[g : g + 1, hp * 256 : hp * 256 + 256]

    crossing(0)
    for part in range(3):
        project(128 * part)
    crossing(1)
    crossing(2)

    tiles = [(hp, pair, 0) for hp in range(4) for pair in range(2)]
    tiles += [(hp, pair, k) for hp in range(4) for k in range(1, 4) for pair in range(2)]

    def stage(i):
        hp, pair, k = tiles[i % 32]
        for q, unit in enumerate(units):
            w = full[hp % 2, k, :, hp // 2, :, 2 * pair + q, 16:48, :].reshape(256, 256)
            unit.push(w, i % 2)

    def multiply(src, first, last, ahead=True):
        for i in range(first, last):
            if ahead or i + 1 < last:
                stage(i + 1)
            hp, pair, k = tiles[i]
            h = src[:, 256 * k : 256 * k + 256]
            for unit in units:
                pltpu.matmul_acc_lhs(unit.gates[2 * hp + pair], h, load_staged_rhs=i % 2)
            h = jnp.concatenate([h, h, h], axis=0)
            for unit in units:
                pltpu.matmul_acc_lhs(unit.spare, h)

    def settle(t, hp, dst, save):
        rows = pl.ds(pl.multiple_of(t * seqs, seqs), seqs)
        alive = keep[t + 1]
        alive = jnp.concatenate([alive, alive], axis=1)
        gate = [pltpu.matmul_pop(units[g % 2].gates[2 * hp + g // 2]) for g in range(4)]
        gate = [gate[g] + pre[hp * 4 + g, rows, :] for g in range(4)]
        cols = slice(hp * 256, hp * 256 + 256)
        c = sigmoid(gate[1]) * cell[:, cols] + sigmoid(gate[0]) * jnp.tanh(gate[2])
        new = sigmoid(gate[3]) * jnp.tanh(c)
        cell[:, cols] = c * alive
        dst[:, cols] = (new * alive).astype(BF16)
        if save:
            learned[head, t - 7, :, cols] = new.astype(BF16)

    def step(t, src, dst, save, begin=False, ahead=True, between=None):
        multiply(src, 0, 6)
        if not begin:
            settle(t - 1, 3, src, save)
        multiply(src, 6, 12)
        if between is not None:
            between()
        multiply(src, 12, 20)
        settle(t, 0, dst, save)
        multiply(src, 20, 26)
        settle(t, 1, dst, save)
        multiply(src, 26, 32, ahead)
        settle(t, 2, dst, save)

    def route(kind, i, owner, to):
        ref = learned.at[head_of(owner), i + 1]
        return pltpu.make_async_remote_copy(
            src_ref=ref,
            dst_ref=ref,
            send_sem=route_send.at[kind, i],
            recv_sem=route_recv.at[kind, i],
            device_id=device(to),
            device_id_type=MESH,
        )

    def send_out(i):
        route(1, i, me, facing).start()
        route(0, i, me, other).start()

    def hand_on(i):
        route(1, i, me, facing).wait_recv()
        route(2, i, facing, other).start()

    def burn(i, _):
        step(2 * i, even, odd, False)
        step(2 * i + 1, odd, even, False)
        return 0

    lag = 6

    def learn(i, _):
        stage(0)
        for u in range(4):
            at = 4 * i + u

            def exchange():
                if u:
                    send_out(at - 1)
                else:

                    @pl.when(i > 0)
                    def _():
                        send_out(at - 1)

                @pl.when(at >= lag)
                def _():
                    hand_on(at - lag)

            src, dst = (odd, even) if u % 2 else (even, odd)
            step(at + 8, src, dst, True, ahead=u < 3, between=exchange)

        @pl.when(i < 3)
        def _():
            project(pl.multiple_of((4 * i + 12) * seqs, 128))

        return 0

    stage(0)
    step(0, even, odd, False, begin=True)
    step(1, odd, even, False)
    lax.fori_loop(1, 3, burn, 0)
    step(6, even, odd, False)
    step(7, odd, even, False, ahead=False)
    lax.fori_loop(0, 4, learn, 0)
    settle(23, 3, even, True)
    send_out(15)
    for unit in units:
        pltpu.matmul_pop(unit.spare)

    def pack(turn, s, half):
        at = pl.ds(pl.multiple_of((2 * s + half) * 16, 16), 16)
        for n in range(4):
            unit, cols = units[n % 2], slice(256 * n, 256 * n + 256)
            rows = learned[s, 8 * half + 1 : 8 * half + 9, :, cols].reshape(256, 256)
            got = pltpu.matmul_pop(unit.run(unit.wide[2 * turn + n // 2], [(pick[s], rows)]))
            packed[:, at, cols] = got.astype(BF16).reshape(8, 16, 256)

    for i in range(16 - lag, 13):
        hand_on(i)
    for load in weights:
        load.wait()
    for i in range(16):
        route(0, i, me, other).wait_recv()
    for half in range(2):
        pack(0, head_of(me), half)
        pack(1, head_of(other), half)
    for i in range(13, 16):
        hand_on(i)
    for half in range(2):
        for i in range(8 * half, 8 * half + 8):
            route(2, i, facing, other).wait_recv()
        pack(0, head_of(facing), half)
        pack(1, head_of(diagonal), half)
    valid_lane = iota((128, 128), 1) < ACTIONS
    def inner(p):
        accs = []
        for n in range(4):
            unit, cols = units[n % 2], slice(256 * n, 256 * n + 256)
            pairs = [
                (packed[p, :, 256 * k : 256 * k + 256], hidden_w[p, 256 * k : 256 * k + 256, cols])
                for k in range(4)
            ]
            accs.append(unit.run(unit.wide[2 * (p % 2) + n // 2], pairs))
        return accs

    def outer(p, accs):
        mid = [jnp.maximum(pltpu.matmul_pop(acc), 0.0).astype(BF16) for acc in accs]
        nil = jnp.zeros((256, 128), BF16)
        pairs = []
        for k in range(4):
            part = slice(256 * (k % 2), 256 * (k % 2) + 256)
            if k < 2:
                tile = [value_w[p, part, :], nil]
            else:
                tile = [adv_w[p, part, :]] * 2
            pairs.append((mid[k], jnp.concatenate(tile, axis=1)))
        unit = units[p % 2]
        got = pltpu.matmul_pop(unit.run(unit.wide[4], pairs))
        mean = jnp.sum(got[:, 128:256], axis=1, keepdims=True) * (1.0 / ACTIONS)
        return jnp.where(valid_lane, got[:, 0:128] - mean, 0.0)

    ready = inner(0)
    for quad in range(2):
        total = None
        for j in range(4):
            p = 4 * quad + j
            now, ready = ready, inner(p + 1) if p < 7 else None
            q = outer(p, now)
            if j:
                q = pltpu.roll(q, 32 * j, 1)
            total = q if total is None else total + q
        for s in range(4):
            answers[s, 32 * quad : 32 * quad + 32, :] = total[32 * s : 32 * s + 32].astype(BF16)
    replies[head] = answers[head]
    back = []
    for to in (diagonal, facing, other):
        back.append(copies.send(answers.at[head_of(to)], replies.at[head], to))
    for copy in back:
        copy.wait_recv()
    got = replies[...].reshape(256, 128).astype(F32).T.astype(BF16)
    found = [
        pltpu.matmul_pop(unit.run(unit.wide[0], [(got, spread[:, 256 * n : 256 * n + 256])]))
        for n, unit in enumerate(units)
    ]
    found = jnp.concatenate(found, axis=1) * group[...]
    found = found[0:32] + found[32:64] + found[64:96] + found[96:128]
    chosen = jnp.where(iota((32, 512), 0).astype(F32) == act[0:1, :], found, 0.0)
    taken = jnp.sum(chosen, axis=0, keepdims=True)
    for t in range(16):
        tile, off = t // 4 * 128, t % 4 * 32
        now = found[0:24, tile : tile + 128]
        mine = jnp.broadcast_to(taken[:, tile : tile + 128], (8, 128))
        if off:
            now = pltpu.roll(now, 128 - off, 1)
            mine = pltpu.roll(mine, 128 - off, 1)
        q_out[pl.ds(t, ACTIONS, stride=16), :] = now[0:ACTIONS, 0:32]
        taken_out[t : t + 1, :] = mine[0:1, 0:32]
    for i in range(16):
        route(0, i, me, other).wait_send()
        route(1, i, me, facing).wait_send()
        route(2, i, facing, other).wait_send()
    for copy in copies.sent:
        copy.wait_send()


def shards(
    features,
    state_h,
    state_c,
    valid,
    ends,
    policy,
    actions,
    w_input,
    w_recur,
    lstm_bias,
    w_hidden,
    w_value,
    w_advantage,
):
    vmem = pl.BlockSpec(memory_space=pltpu.VMEM)
    held = [(16, 4, 256), (32, 4, 256), (24, 32), (16, 32), (1, 32), (1, 32), (4, 1024), (8, 512), (ACTIONS, 8, 512)]
    held += [(32, 1024), (32, 1024)]
    kinds = [BF16] * 2 + [jnp.int32] * 4 + [F32] + [BF16] * 4
    dma = pltpu.SemaphoreType.DMA
    given = (
        w_input,
        w_recur,
        ends.T,
        actions.T,
        policy.T,
        valid[None, :],
        lstm_bias,
        w_value,
        w_advantage.transpose(2, 0, 1),
        state_h,
        state_c,
        features.reshape(6, 128, features.shape[2]),
        w_hidden,
    )
    pinned = [pltpu.with_memory_space_constraint(v, pltpu.HBM) for v in given]
    q, taken = pl.pallas_call(
        core_kernel,
        out_shape=(
            jax.ShapeDtypeStruct((ACTIONS * 16, 32), F32),
            jax.ShapeDtypeStruct((16, 32), F32),
        ),
        in_specs=[pl.BlockSpec(memory_space=pltpu.HBM)] * 13,
        out_specs=(vmem, vmem),
        scratch_shapes=[pltpu.VMEM(shape, kind) for shape, kind in zip(held, kinds)]
        + [
            pltpu.VMEM((4, 48, 256), BF16),
            pltpu.VMEM((2, 4, 2, 2, 4, 4, 48, 256), BF16),
            pltpu.VMEM((16, 768, 256), F32),
            pltpu.VMEM((32, 1024), BF16),
            pltpu.VMEM((32, 1024), BF16),
            pltpu.VMEM((32, 1024), F32),
            pltpu.VMEM((25, 32, 128), F32),
            pltpu.VMEM((768, 512), BF16),
            pltpu.VMEM((8, 1024, 1024), BF16),
            pltpu.VMEM((4, 17, 32, 1024), BF16),
            pltpu.VMEM((8, 128, 1024), BF16),
            pltpu.VMEM((128, 128), F32),
            pltpu.VMEM((1024, 128), F32),
            pltpu.VMEM((4, 16, 256), F32),
            pltpu.VMEM((4, 128, 256), BF16),
            pltpu.VMEM((8, 512, 128), BF16),
            pltpu.VMEM((8, 512, 128), BF16),
            pltpu.VMEM((256, 512), BF16),
            pltpu.VMEM((128, 512), F32),
            pltpu.VMEM((8, 512), F32),
            pltpu.VMEM((4, 64, 128), BF16),
            pltpu.VMEM((4, 64, 128), BF16),
            dma((20,)),
            dma((SENDS,)),
            dma((SENDS,)),
            dma((3, 16)),
            dma((3, 16)),
        ],
        compiler_params=pltpu.CompilerParams(
            collective_id=0, has_side_effects=True, vmem_limit_bytes=int(53.5 * 2**20)
        ),
        name="core",
    )(*pinned)
    return q.reshape(ACTIONS, 16, 32).transpose(2, 1, 0), taken.T


def solution(mesh):
    return jax.shard_map(
        shards,
        mesh=mesh,
        in_specs=(
            P(("batch", "head"), None, None),
            P(("batch", "head"), None),
            P(("batch", "head"), None),
            P(("batch", "head")),
            P(("batch", "head"), None),
            P(("batch", "head"), None),
            P(("batch", "head"), None),
            P("batch", None, "head"),
            P("batch", None, "head"),
            P(),
            P("head", None, None),
            P("head", None),
            P("head", None, None),
        ),
        out_specs=(P(("batch", "head"), None, None), P(("batch", "head"), None)),
        check_vma=False,
    )
```
